32 devices in a mesh: curve: 8 (over z, y), sub: 4 (over x, core).
Axes of the slice: x: 2, y: 2, z: 4, core: 2. Of those that a mesh axis runs over, the one named last changes fastest.
Arguments:
- prognostic: float32 [4, 192, 32, 4, 4, 128], P(None, 'curve', 'sub'), may hold values from -6 to 6
- layer_mass: float32 [192, 32, 4, 4, 128], P('curve', 'sub'), may hold values from 0.5 to 2
- column_aux: bfloat16 [49152, 1013], P(('curve', 'sub')), may hold values from -6 to 6
- group_owner: int32 [24576, 1], P(('curve', 'sub')), may hold values from 0 to 31; in each aligned block of 768 rows (0 to 767, 768 to 1535, ...) at most 48 rows name the same one
- weight_in: bfloat16 [1525, 2048], replicated, may hold values from -0.15625 to 0.15625
- bias_in: float32 [2048], replicated, may hold values from -3 to 3
- weight_out: bfloat16 [2048, 512], replicated, may hold values from -0.125 to 0.125
- bias_out: float32 [512], replicated, may hold values from -2 to 2
Outputs:
- advanced: float32 [4, 192, 32, 4, 4, 128], P(None, 'curve', 'sub')
The draws below stay inside these ranges and needn't reach their ends.
Inputs may be any that keep to these rules, and one draw needn't show every extreme that they name: `group_owner`: among the 768 columns of one device, at most 48 name the same owner, and every device owns some column.
All inputs are finite; a program needn't handle non-finite values.
Results may differ from the reference program's by a relative error of at most 0.0035.
Values may be sent and summed in bfloat16 or wider, within the bound.
No kernel may reach another device: no remote copies, remote signals or barrier semaphores. Data moves between devices by JAX's collectives and lax.ppermute only.
A program may use at most 128 MiB of HBM per device.

```python
import math
import jax
import jax.numpy as jnp
import numpy as np
from jax import lax

NV = 4
LEV = 128
F_IN = 1525
HID = 2048
EA = 24
EB = 8
AUX = 1013
COL_DEV = 768
COLUMNS = 24576
CAP = 48
NEA = 192
NEB = 32
N_CURVE = 8
N_SUB = 4
DEVICES = 32


def level_of(key, dims, cuts, low, top_value):
    gain = 1.0
    for dim, blocks in cuts:
        heights = jax.random.uniform(jax.random.fold_in(jax.random.fold_in(key, 6), dim), (blocks,), jnp.float32, low / len(cuts), top_value / len(cuts))
        gain = gain * jnp.repeat(jnp.exp(heights), dims[dim] // blocks).reshape((-1,) + (1,) * (len(dims) - 1 - dim))
    return gain


def routed_block(rng, own, number, rows, number_of, top, bound, slope):
    order = jax.random.permutation(rng, number_of)
    packed, usual = shares(number_of, rows * top, bound, slope, True), shares(number_of, rows * top, bound, slope, False)
    places = jnp.arange(number_of)

    def named(sizes, offset_by):
        used = int((sizes > 0).sum())
        fixed = max(1, used // 4)
        shifted = fixed + (places - fixed + offset_by * (used - fixed)) % max(1, number_of - fixed)
        return jnp.zeros((number_of,), jnp.int32).at[order[jnp.where(places < fixed, places, shifted)]].set(jnp.asarray(sizes, jnp.int32))

    sizes = jnp.where(number % 4 == 0, named(packed, number // 4), named(usual, number - number // 4 - 1))
    mixed = jax.random.permutation(jax.random.fold_in(own, 3), number_of)
    donor, sink = mixed[0:number_of // 2 * 2:2], mixed[1:number_of // 2 * 2:2]
    room = jnp.minimum(sizes[donor] - 1, bound - sizes[sink]) // 2
    room = jnp.where((donor == order[0]) | (sink == order[0]) | (sizes[sink] == 0), 0, jnp.maximum(room, 0))
    shifted = jax.random.randint(jax.random.fold_in(own, 4), (number_of // 2,), 0, 1 << 20) % (room + 1)
    sizes = sizes.at[donor].add(-shifted).at[sink].add(shifted)
    members = jnp.searchsorted(jnp.cumsum(sizes), jnp.arange(rows * top), side="right").astype(jnp.int32)
    grid = members.reshape(top, rows).T
    grid = grid[jax.random.permutation(jax.random.fold_in(own, 1), rows)]
    offset_by = jax.random.randint(jax.random.fold_in(own, 2), (rows, 1), 0, top)
    return jnp.take_along_axis(grid, (jnp.arange(top)[None, :] + offset_by) % top, axis=1)


def shares(count, total, most, skew, full):
    portions = [(1 << 20) // math.isqrt(rank ** skew) + 1 for rank in range(1, count + 1)]
    largest = most if full else min(most, max(-(-total // count), total * portions[0] // sum(portions)))
    least = 1 if total - largest >= count - 1 else 0
    holding, rest = [largest] + [least] * (count - 1), total - largest - least * (count - 1)
    while rest > 0:
        candidates = [i for i in range(1, count) if holding[i] < largest] or [i for i in range(1, count) if holding[i] < most]
        whole, budget = sum([portions[i] for i in candidates]), rest
        for i in candidates:
            extra = min(most - holding[i], max(1, budget * portions[i] // whole), rest)
            holding[i] = holding[i] + extra
            rest = rest - extra
    return np.array(holding)


def bell_draw(rng, dims, spread, reach, cuts=(), kind=jnp.bfloat16):
    factor_of = level_of(rng, dims, cuts, -0.22, 0.18) if cuts else 1.0
    result = jax.random.normal(rng, dims, jnp.float32) * spread * factor_of
    return jnp.minimum(jnp.maximum(result, -reach), reach).astype(kind)


def setup_inputs(seed: int = 0) -> dict:
    streams_of = jax.random.split(jax.random.key(seed), 9)
    prognostic = bell_draw(streams_of[0], (NV, NEA, NEB, 4, 4, LEV), 1.0, 6.0, ((1, 8), (2, 4)), jnp.float32)
    layer_mass = jnp.clip(jnp.exp(math.log(2.0) - 1.3862944 * jax.random.uniform(streams_of[1], (NEA, NEB, 4, 4, LEV), jnp.float32) ** level_of(streams_of[1], (NEA, NEB, 4, 4, LEV), ((0, 8), (1, 4)), -0.2, 0.2)), 0.5, 2.0)
    column_aux = bell_draw(streams_of[2], (DEVICES * DEVICES * CAP, AUX), 1.0, 6.0, ((0, 32),))
    group_owner_keys = jax.random.split(jax.random.fold_in(streams_of[3], 1), COLUMNS // COL_DEV)
    group_owner_turns = jax.random.permutation(jax.random.fold_in(streams_of[3], 3), COLUMNS // COL_DEV)
    group_owner = jax.vmap(lambda own, number: routed_block(jax.random.fold_in(streams_of[3], 2), own, number, COL_DEV, DEVICES, 1, CAP, 2))(group_owner_keys, group_owner_turns).reshape((COLUMNS, 1))
    weight_in = bell_draw(streams_of[4], (F_IN, HID), F_IN ** -0.5, 0.15625)
    bias_in = bell_draw(streams_of[5], (HID,), 0.5, 3.0, (), jnp.float32)
    weight_out = bell_draw(streams_of[6], (HID, NV * LEV), HID ** -0.5, 0.125)
    bias_out = bell_draw(streams_of[7], (NV * LEV,), 0.3, 2.0, (), jnp.float32)
    return {"prognostic": prognostic, "layer_mass": layer_mass, "column_aux": column_aux, "group_owner": group_owner, "weight_in": weight_in, "bias_in": bias_in, "weight_out": weight_out, "bias_out": bias_out}


section_step = 0.1

def node_tables():
    nodes = np.array([-1.0, -1.0 / np.sqrt(5.0), 1.0 / np.sqrt(5.0), 1.0])
    quadrature = np.array([1.0 / 6.0, 5.0 / 6.0, 5.0 / 6.0, 1.0 / 6.0])
    products = np.array([np.prod([nodes[left_node] - nodes[other_node] for other_node in range(4) if other_node != left_node]) for left_node in range(4)])
    derivative = np.zeros((4, 4))
    for left_node in range(4):
        for other_node in range(4):
            if left_node != other_node:
                derivative[left_node, other_node] = products[left_node] / (products[other_node] * (nodes[left_node] - nodes[other_node]))
            else:
                derivative[left_node, left_node] = sum((1.0 / (nodes[left_node] - nodes[third_node]) for third_node in range(4) if third_node != left_node))
    return (derivative.astype(np.float32), quadrature.astype(np.float32))

def advect(prognostic, derivative):
    along_first = jnp.einsum('ik,fabkjl->fabijl', derivative, prognostic, precision=lax.Precision.HIGHEST)
    along_second = jnp.einsum('jk,fabikl->fabijl', derivative, prognostic, precision=lax.Precision.HIGHEST)
    return -(prognostic[0:1] * along_first + prognostic[1:2] * along_second)

def node_mass(layer_mass, quadrature):
    return quadrature[:, None, None] * quadrature[None, :, None] * layer_mass

def cell_average(prognostic, node_weight):
    fields = prognostic.shape[0]
    rows_a, rows_b, levels = (node_weight.shape[0], node_weight.shape[1], node_weight.shape[4])
    weighted = (prognostic * node_weight[None]).reshape(fields, rows_a, rows_b, 2, 2, 2, 2, levels)
    weighted_sum = lax.optimization_barrier(jnp.sum(weighted, axis=(4, 6)))
    mass_sum = lax.optimization_barrier(jnp.sum(node_weight.reshape(rows_a, rows_b, 2, 2, 2, 2, levels), axis=(3, 5)))
    return weighted_sum / mass_sum[None]

def spread_cells(cells):
    return jnp.repeat(jnp.repeat(cells, 2, axis=3), 2, axis=4)

def apply_network(inputs, weight_in, bias_in, weight_out, bias_out):
    hidden = jax.nn.silu(jnp.dot(inputs, weight_in, preferred_element_type=jnp.float32) + bias_in).astype(jnp.bfloat16)
    return (jnp.dot(hidden, weight_out, preferred_element_type=jnp.float32) + bias_out).astype(jnp.bfloat16)

def reference(prognostic, layer_mass, column_aux, group_owner, weight_in, bias_in, weight_out, bias_out):
    derivative_np, quadrature_np = node_tables()
    derivative = jnp.asarray(derivative_np)
    quadrature = jnp.asarray(quadrature_np)
    advection = advect(prognostic, derivative)
    node_weight = node_mass(layer_mass, quadrature)
    stacked = jnp.concatenate([advection * node_weight[None], node_weight[None]], axis=0)
    following = jnp.roll(stacked, -1, axis=1)
    preceding = jnp.roll(stacked, 1, axis=1)
    passed = stacked.at[:, :, :, 3].add(following[:, :, :, 0]).at[:, :, :, 0].add(preceding[:, :, :, 3])
    following = jnp.roll(passed, -1, axis=2)
    preceding = jnp.roll(passed, 1, axis=2)
    summed = passed.at[:, :, :, :, 3].add(following[:, :, :, :, 0]).at[:, :, :, :, 0].add(preceding[:, :, :, :, 3])
    section = prognostic + section_step * (summed[:NV] / summed[NV:])
    cells = cell_average(prognostic, node_weight)
    state_cols = cells.reshape(NV, N_CURVE, EA, N_SUB, EB, 2, 2, LEV).transpose(1, 3, 2, 4, 5, 6, 0, 7)
    state_cols = state_cols.reshape(COLUMNS, NV * LEV).astype(jnp.bfloat16)
    targets = group_owner[:, 0].reshape(DEVICES, COL_DEV)
    hits = (targets[:, :, None] == jnp.arange(DEVICES, dtype=jnp.int32)[None, None]).astype(jnp.int32)
    earlier = (jnp.cumsum(hits, axis=1) - hits).astype(jnp.int32)
    slot_index = lax.optimization_barrier(jnp.sum(hits * earlier, axis=2)).astype(jnp.int32)
    source = jnp.arange(DEVICES, dtype=jnp.int32)[:, None]
    aux_rows = (targets * (DEVICES * CAP) + source * CAP + slot_index).reshape(COLUMNS).astype(jnp.int32)
    aux_cols = column_aux[aux_rows]
    increment = apply_network(jnp.concatenate([state_cols, aux_cols], axis=1), weight_in, bias_in, weight_out, bias_out)
    back = increment.reshape(N_CURVE, N_SUB, EA, EB, 2, 2, NV, LEV).transpose(6, 0, 2, 1, 3, 4, 5, 7)
    back = back.reshape(NV, NEA, NEB, 2, 2, LEV)
    return section + spread_cells(back.astype(jnp.float32))
```

```python
import jax
import jax.numpy as jnp
import numpy as np
from jax import lax
from jax.experimental import pallas as pl
from jax.experimental.pallas import tpu as pltpu
from jax.sharding import PartitionSpec as P

section_step = 0.1
AXES = ("curve", "sub")
F32 = jnp.float32
BF16 = jnp.bfloat16


def node_tables():
    nodes = np.array([-1.0, -1.0 / np.sqrt(5.0), 1.0 / np.sqrt(5.0), 1.0])
    quadrature = np.array([1.0 / 6.0, 5.0 / 6.0, 5.0 / 6.0, 1.0 / 6.0])
    products = np.array(
        [np.prod([nodes[i] - nodes[k] for k in range(4) if k != i]) for i in range(4)]
    )
    derivative = np.zeros((4, 4))
    for i in range(4):
        for k in range(4):
            if i != k:
                derivative[i, k] = products[i] / (products[k] * (nodes[i] - nodes[k]))
            else:
                derivative[i, i] = sum(1.0 / (nodes[i] - nodes[m]) for m in range(4) if m != i)
    return derivative.astype(np.float32), quadrature.astype(np.float32)


def row_tables():
    d, w = node_tables()
    s = np.arange(8)
    i, j = s // 4, s % 4
    tables = []
    for half in (0, 2):
        for column in (i, 1 - i, 2 + i, 3 - i):
            tables.append(-d[half + i, column])
    for shift in range(4):
        tables.append(-d[j, (j - shift) % 4])
    for half in (0, 2):
        tables.append(w[half + i] * w[j])
    return np.repeat(np.stack(tables)[:, :, None], 128, axis=2).astype(np.float32)


def lane_rows(x):
    return lax.broadcasted_iota(jnp.int32, x, len(x) - 2)


def roll(x, shift):
    return pltpu.roll(x, shift % 8, axis=1)


def turn_body(x_ref, o_ref):
    n = x_ref.shape[1]
    width = x_ref.shape[0]
    eye = (
        lax.broadcasted_iota(jnp.int32, (n, n), 0) == lax.broadcasted_iota(jnp.int32, (n, n), 1)
    ).astype(BF16)
    y = lax.dot_general(eye, x_ref[...], (((1,), (1,)), ((), ())), preferred_element_type=F32)
    o_ref[:, :width] = y.astype(BF16)
    o_ref[:, width:] = jnp.zeros((n, o_ref.shape[1] - width), BF16)


def turn(aux_t, padded):
    width, rows = aux_t.shape
    block = 256
    return pl.pallas_call(
        turn_body,
        grid=(rows // block,),
        in_specs=[pl.BlockSpec((width, block), lambda i: (0, i))],
        out_specs=pl.BlockSpec((block, padded), lambda i: (i, 0)),
        out_shape=jax.ShapeDtypeStruct((rows, padded), BF16),
        name="turn",
    )(aux_t)


def tend_body(x_ref, m_ref, t_ref, pick_ref, o_ref, c_ref):
    fields = x_ref.shape[0]
    rows = x_ref.shape[1]
    group = 128
    sub = lax.broadcasted_iota(jnp.int32, (group // 16, 8, 128), 1) % 4
    tab = [t_ref[k][None] for k in range(14)]

    def step(g, carry):
        at = pl.multiple_of(g * group, group)

        def halves(v):
            v = v.reshape(group // 16, 2, 8, 128)
            return v[:, 0], v[:, 1]

        def keep(f, y0, y1):
            o_ref[f, pl.ds(at, group), :] = jnp.stack([y0, y1], axis=1).reshape(group, 128)

        m0, m1 = halves(m_ref[pl.ds(at, group), :])
        w = (m0 * tab[12], m1 * tab[13])

        def pool(v):
            v = v + roll(v, 4)
            return v + roll(v, 7)

        inv = [1.0 / pool(v) for v in w]
        u = halves(x_ref[0, pl.ds(at, group), :])
        v = halves(x_ref[1, pl.ds(at, group), :])
        uw = (u[0] * w[0], u[1] * w[1])
        vw = (v[0] * w[0], v[1] * w[1])
        for f in range(fields):
            x = u if f == 0 else v if f == 1 else halves(x_ref[f, pl.ds(at, group), :])
            r4 = (roll(x[0], 4), roll(x[1], 4))
            out = []
            means = []
            for h in range(2):
                da = (
                    tab[4 * h] * x[0]
                    + tab[4 * h + 1] * r4[0]
                    + tab[4 * h + 2] * x[1]
                    + tab[4 * h + 3] * r4[1]
                )
                db = tab[8] * x[h]
                for k in (1, 2, 3):
                    turned = jnp.where(sub >= k, roll(x[h], k), roll(r4[h], k))
                    db = db + tab[8 + k] * turned
                out.append(uw[h] * da + vw[h] * db)
                means.append(pool(x[h] * w[h]) * inv[h])
            keep(f, out[0], out[1])
            means = jnp.stack(means, axis=1).reshape(group, 128).astype(BF16)
            c_ref[pl.ds(pl.multiple_of(g * (group // 4), group // 4), group // 4), f * 128 : (f + 1) * 128] = jnp.dot(
                pick_ref[...], means, preferred_element_type=F32
            ).astype(BF16)
        return carry

    lax.fori_loop(0, rows // group, step, 0)


def pick_table(group):
    rows = np.arange(group)
    pick = np.zeros((group // 4, group), np.float32)
    for c in range(group // 4):
        element, p, q = c // 4, (c // 2) % 2, c % 2
        pick[c, element * 16 + p * 8 + q * 2] = 1.0
    return pick


def tendencies(x, mass):
    fields, rows, levels = x.shape
    block = 384
    return pl.pallas_call(
        tend_body,
        grid=(rows // block,),
        in_specs=[
            pl.BlockSpec((fields, block, levels), lambda i: (0, i, 0)),
            pl.BlockSpec((block, levels), lambda i: (i, 0)),
            pl.BlockSpec((14, 8, 128), lambda i: (0, 0, 0)),
            pl.BlockSpec((32, 128), lambda i: (0, 0)),
        ],
        out_specs=[
            pl.BlockSpec((fields, block, levels), lambda i: (0, i, 0)),
            pl.BlockSpec((block // 4, fields * levels), lambda i: (i, 0)),
        ],
        out_shape=[
            jax.ShapeDtypeStruct((fields, rows, levels), F32),
            jax.ShapeDtypeStruct((rows // 4, fields * levels), BF16),
        ],
        name="tendencies",
    )(x, mass, jnp.asarray(row_tables()), jnp.asarray(pick_table(128), BF16))


def section_body(t_ref, x_ref, m_ref, q_ref, top_ref, bottom_ref, left_ref, right_ref, o_ref, inv_ref):
    rows = x_ref.shape[1]
    per = top_ref.shape[1] // 8
    span = per * 16
    count = rows // span
    s = lax.broadcasted_iota(jnp.int32, (per, 8, 128), 1)
    low = s < 4
    first = s % 4 == 0
    last = s % 4 == 3
    zero = jnp.zeros((1, 8, 128), F32)
    f = pl.program_id(0)

    def halves(v):
        v = v.reshape(per, 2, 8, 128)
        return v[:, 0], v[:, 1]

    def sums(a, load, k):
        here = load(a)
        above = load(jnp.maximum(a - 1, 0))[1]
        below = load(jnp.minimum(a + 1, count - 1))[0]
        top = top_ref[k].reshape(per, 8, 128)
        bottom = bottom_ref[k].reshape(per, 8, 128)
        add0 = jnp.where(a == 0, top, jnp.where(low, roll(above, 4), 0.0))
        add1 = jnp.where(a == count - 1, bottom, jnp.where(low, 0.0, roll(below, 4)))
        at = pl.multiple_of(a * 16, 16)
        left = halves_one(left_ref[k, pl.ds(at, 16), :])
        right = halves_one(right_ref[k, pl.ds(at, 16), :])
        result = []
        for h, p in enumerate((here[0] + add0, here[1] + add1)):
            up = jnp.where(last, roll(p, 3), 0.0)
            down = jnp.where(first, roll(p, 5), 0.0)
            up = jnp.concatenate([up_shift(up), right[h]], axis=0)
            down = jnp.concatenate([left[h], down[:-1]], axis=0)
            result.append(p + up + down)
        return result

    def halves_one(v):
        v = v.reshape(1, 2, 8, 128)
        return v[:, 0], v[:, 1]

    def up_shift(v):
        return v[1:]

    def window(a):
        return pl.ds(pl.multiple_of(a * span, span), span)

    def mass_at(a):
        m0, m1 = halves(m_ref[window(a), :])
        return m0 * q_ref[0][None], m1 * q_ref[1][None]

    @pl.when(f == 0)
    def _():
        def step(a, carry):
            w0, w1 = sums(a, mass_at, 4)
            inv_ref[window(a), :] = jnp.stack(
                [section_step / w0, section_step / w1], axis=1
            ).reshape(span, 128)
            return carry

        lax.fori_loop(0, count, step, 0)

    def step(a, carry):
        y0, y1 = sums(a, lambda b: halves(t_ref[0, window(b), :]), f)
        y = jnp.stack([y0, y1], axis=1).reshape(span, 128)
        o_ref[0, window(a), :] = x_ref[0, window(a), :] + y * inv_ref[window(a), :]
        return carry

    lax.fori_loop(0, count, step, 0)


def section_of(t, x, mass, top, bottom, left, right):
    fields, rows, levels = x.shape
    whole = lambda a: pl.BlockSpec(a.shape, lambda f: (0,) * a.ndim)
    quad = jnp.asarray(row_tables()[12:14])
    one = pl.BlockSpec((1, rows, levels), lambda f: (f, 0, 0))
    return pl.pallas_call(
        section_body,
        grid=(fields,),
        in_specs=[one, one] + [whole(a) for a in (mass, quad, top, bottom, left, right)],
        out_specs=one,
        out_shape=jax.ShapeDtypeStruct(x.shape, F32),
        scratch_shapes=[pltpu.VMEM((rows, levels), F32)],
        name="section",
    )(t, x, mass, quad, top, bottom, left, right)


def places_body(owner_ref, o_ref, *, devices, capacity):
    cols = owner_ref.shape[0]
    owner = owner_ref[...]
    hits = owner == lax.broadcasted_iota(jnp.int32, (cols, devices), 1)
    hits = jnp.where(hits, 1.0, 0.0)
    before = lax.broadcasted_iota(jnp.int32, (cols, cols), 0) > lax.broadcasted_iota(
        jnp.int32, (cols, cols), 1
    )
    before = jnp.where(before, 1.0, 0.0).astype(BF16)
    earlier = jnp.dot(before, hits.astype(BF16), preferred_element_type=F32)
    slot = jnp.sum(hits * earlier, axis=1, keepdims=True).astype(jnp.int32)
    place = owner * capacity + slot
    wide = lax.broadcasted_iota(jnp.int32, (cols, devices * capacity), 1)
    o_ref[...] = jnp.where(place == wide, 1.0, 0.0).astype(BF16)


def places(owner, devices, capacity):
    return pl.pallas_call(
        lambda a, o: places_body(a, o, devices=devices, capacity=capacity),
        out_shape=jax.ShapeDtypeStruct((owner.shape[0], devices * capacity), BF16),
        name="places",
    )(owner)


def first_body(s_ref, w_ref, b_ref, o_ref):
    o_ref[...] = jnp.dot(s_ref[...], w_ref[...], preferred_element_type=F32) + b_ref[...]


def first_part(state, weight, bias):
    cols, width = state.shape
    hidden = weight.shape[1]
    block = 512
    return pl.pallas_call(
        first_body,
        grid=(hidden // block,),
        in_specs=[
            pl.BlockSpec((cols, width), lambda i: (0, 0)),
            pl.BlockSpec((width, block), lambda i: (0, i)),
            pl.BlockSpec((1, block), lambda i: (0, i)),
        ],
        out_specs=pl.BlockSpec((cols, block), lambda i: (0, i)),
        out_shape=jax.ShapeDtypeStruct((cols, hidden), F32),
        name="first_part",
    )(state, weight, bias)


def finish_body(sel_ref, aux_ref, w_ref, part_ref, wo_ref, bo_ref, spread_ref, x_ref, o_ref):
    fields = x_ref.shape[0]
    levels = x_ref.shape[2]
    aux = jnp.dot(sel_ref[...], aux_ref[...], preferred_element_type=F32).astype(BF16)
    v = part_ref[...] + jnp.dot(aux, w_ref[...], preferred_element_type=F32)
    hidden = (v / (1.0 + jnp.exp(-v))).astype(BF16)
    inc = jnp.dot(hidden, wo_ref[...], preferred_element_type=F32) + bo_ref[...]
    inc = inc.astype(BF16)
    group = spread_ref.shape[1]
    for g in range(inc.shape[0] // group):
        wide = jnp.dot(
            spread_ref[...], inc[g * group : (g + 1) * group], preferred_element_type=F32
        )
        at = pl.ds(g * group * 4, group * 4)
        for f in range(fields):
            o_ref[f, at, :] = x_ref[f, at, :] + wide[:, f * levels : (f + 1) * levels]


def spread_table(group):
    spread = np.zeros((group * 4, group), np.float32)
    for r in range(group * 4):
        e, i, j = r // 16, (r // 4) % 4, r % 4
        spread[r, e * 4 + (i // 2) * 2 + j // 2] = 1.0
    return spread


def finish(sel, aux, weight, part, weight_out, bias_out, x):
    cols, slots = sel.shape
    fields, rows, levels = x.shape
    block = 256
    spread = jnp.asarray(spread_table(128), BF16)
    whole = lambda a: pl.BlockSpec(a.shape, lambda i: (0,) * a.ndim)
    return pl.pallas_call(
        finish_body,
        grid=(cols // block,),
        in_specs=[
            pl.BlockSpec((block, slots), lambda i: (i, 0)),
            whole(aux),
            whole(weight),
            pl.BlockSpec((block, weight.shape[1]), lambda i: (i, 0)),
            whole(weight_out),
            whole(bias_out),
            whole(spread),
            pl.BlockSpec((fields, block * 4, levels), lambda i: (0, i, 0)),
        ],
        out_specs=pl.BlockSpec((fields, block * 4, levels), lambda i: (0, i, 0)),
        out_shape=jax.ShapeDtypeStruct(x.shape, F32),
        name="finish",
    )(sel, aux, weight, part, weight_out, bias_out, spread, x)


def shards(
    prognostic, layer_mass, column_aux, group_owner, weight_in, bias_in, weight_out, bias_out
):
    fields, rows_a, rows_b, _, _, levels = prognostic.shape
    n_curve, n_sub = lax.axis_size("curve"), lax.axis_size("sub")
    devices = n_curve * n_sub
    capacity = column_aux.shape[0] // devices
    aux_width = column_aux.shape[1]
    padded = -(-aux_width // 128) * 128
    state_width = fields * levels
    rows = rows_a * rows_b * 16

    home = turn(column_aux.T, padded).reshape(devices, capacity, padded)
    home = lax.all_to_all(home, AXES, split_axis=0, concat_axis=0, tiled=True)
    home = home.reshape(devices * capacity, padded)

    x = prognostic.reshape(fields, rows, levels)
    mass = layer_mass.reshape(rows, levels)
    tend, state = tendencies(x, mass)

    quadrature = node_tables()[1]
    def ahead(n):
        return [(i, (i + 1) % n) for i in range(n)]
    def back(n):
        return [((i + 1) % n, i) for i in range(n)]

    t6 = tend.reshape(fields, rows_a, rows_b, 4, 4, levels)
    w_edge = (quadrature[0] * quadrature)[:, None]
    head = jnp.concatenate([t6[:, 0, :, 0], (layer_mass[0, :, 0] * w_edge)[None]], axis=0)
    tail = jnp.concatenate([t6[:, -1, :, 3], (layer_mass[-1, :, 3] * w_edge)[None]], axis=0)
    above = lax.ppermute(tail.astype(BF16), "curve", ahead(n_curve)).astype(F32)
    below = lax.ppermute(head.astype(BF16), "curve", back(n_curve)).astype(F32)
    top = jnp.pad(above, ((0, 0), (0, 0), (0, 4), (0, 0))).reshape(fields + 1, rows_b * 8, levels)
    bottom = jnp.pad(below, ((0, 0), (0, 0), (4, 0), (0, 0))).reshape(fields + 1, rows_b * 8, levels)

    def edge(b, j):
        e = jnp.concatenate(
            [t6[:, :, b, :, j], (layer_mass[:, b, :, j] * (quadrature[j] * quadrature)[:, None])[None]],
            axis=0,
        )
        before = jnp.concatenate([above[:, None, b, j], e[:, :-1, 3]], axis=1)
        after = jnp.concatenate([e[:, 1:, 0], below[:, None, b, j]], axis=1)
        return jnp.stack([e[:, :, 0] + before, e[:, :, 1], e[:, :, 2], e[:, :, 3] + after], axis=2)

    right_out = edge(rows_b - 1, 3)
    left_out = edge(0, 0)
    left = lax.ppermute(right_out.astype(BF16), "sub", ahead(n_sub)).astype(F32)
    right = lax.ppermute(left_out.astype(BF16), "sub", back(n_sub)).astype(F32)
    left = jnp.pad(left[:, :, :, None], ((0, 0), (0, 0), (0, 0), (0, 3), (0, 0)))
    right = jnp.pad(right[:, :, :, None], ((0, 0), (0, 0), (0, 0), (3, 0), (0, 0)))
    left = left.reshape(fields + 1, rows_a * 16, levels)
    right = right.reshape(fields + 1, rows_a * 16, levels)
    section = section_of(tend, x, mass, top, bottom, left, right)

    sel = places(group_owner, devices, capacity)
    part = first_part(state, weight_in[:state_width], bias_in[None])
    weight_aux = jnp.pad(weight_in[state_width:], ((0, padded - aux_width), (0, 0)))
    out = finish(sel, home, weight_aux, part, weight_out, bias_out[None], section)
    return out.reshape(prognostic.shape)


def solution(mesh):
    return jax.shard_map(
        shards,
        mesh=mesh,
        in_specs=(
            P(None, "curve", "sub", None, None, None),
            P("curve", "sub", None, None, None),
            P(("curve", "sub"), None),
            P(("curve", "sub"), None),
            P(),
            P(),
            P(),
            P(),
        ),
        out_specs=P(None, "curve", "sub", None, None, None),
        check_vma=False,
    )
```

```python
import jax
import jax.numpy as jnp
import numpy as np
from jax import lax
from jax.experimental import pallas as pl
from jax.experimental.pallas import tpu as pltpu
from jax.sharding import PartitionSpec as P

section_step = 0.1
AXES = ("curve", "sub")
F32 = jnp.float32
BF16 = jnp.bfloat16


def node_tables():
    nodes = np.array([-1.0, -1.0 / np.sqrt(5.0), 1.0 / np.sqrt(5.0), 1.0])
    quadrature = np.array([1.0 / 6.0, 5.0 / 6.0, 5.0 / 6.0, 1.0 / 6.0])
    products = np.array(
        [np.prod([nodes[i] - nodes[k] for k in range(4) if k != i]) for i in range(4)]
    )
    derivative = np.zeros((4, 4))
    for i in range(4):
        for k in range(4):
            if i != k:
                derivative[i, k] = products[i] / (products[k] * (nodes[i] - nodes[k]))
            else:
                derivative[i, i] = sum(1.0 / (nodes[i] - nodes[m]) for m in range(4) if m != i)
    return derivative.astype(np.float32), quadrature.astype(np.float32)


def row_tables():
    d, w = node_tables()
    s = np.arange(8)
    i, j = s // 4, s % 4
    tables = []
    for half in (0, 2):
        for column in (i, 1 - i, 2 + i, 3 - i):
            tables.append(-d[half + i, column])
    for shift in range(4):
        tables.append(-d[j, (j - shift) % 4])
    for half in (0, 2):
        tables.append(w[half + i] * w[j])
    return np.repeat(np.stack(tables)[:, :, None], 128, axis=2).astype(np.float32)


def lane_rows(x):
    return lax.broadcasted_iota(jnp.int32, x, len(x) - 2)


def roll(x, shift):
    return pltpu.roll(x, shift % 8, axis=1)


def turn_body(x_ref, o_ref):
    width = x_ref.shape[0]
    o_ref[:, :width] = x_ref[...].T
    o_ref[:, width:] = jnp.zeros((o_ref.shape[0], o_ref.shape[1] - width), BF16)


def turn(aux_t, padded):
    width, rows = aux_t.shape
    block = rows // 2
    return pl.pallas_call(
        turn_body,
        grid=(rows // block,),
        in_specs=[pl.BlockSpec((width, block), lambda i: (0, i))],
        out_specs=pl.BlockSpec((block, padded), lambda i: (i, 0)),
        out_shape=jax.ShapeDtypeStruct((rows, padded), BF16),
        name="turn",
        compiler_params=pltpu.CompilerParams(vmem_limit_bytes=60 << 20),
    )(aux_t)


def tend_body(x_ref, m_ref, t_ref, pick_ref, o_ref, c_ref, l_ref, r_ref, mean_ref, *, per):
    fields = x_ref.shape[0]
    rows = x_ref.shape[1]
    span = per * 16
    part = 4
    group = part * 16
    sub = lax.broadcasted_iota(jnp.int32, (part, 8, 128), 1) % 4
    row8 = lax.broadcasted_iota(jnp.int32, (8, 128), 0) % 4
    tab = [t_ref[k][None] for k in range(14)]

    def step(a, carry):
        edge_at = pl.ds(pl.multiple_of(a * 8, 8), 8)
        for q in range(per // part):
            at = pl.ds(pl.multiple_of(a * span + q * group, group), group)

            def halves(v):
                v = v.reshape(part, 2, 8, 128)
                return v[:, 0], v[:, 1]

            def edges(f, y):
                if q == 0:
                    p = jnp.where(row8 == 0, y[0][0], 0.0) + jnp.where(
                        row8 == 1, pltpu.roll(y[1][0], 1, axis=0), 0.0
                    )
                    l_ref[f, edge_at, :] = p.astype(BF16)
                if q == per // part - 1:
                    p = jnp.where(row8 == 0, pltpu.roll(y[0][part - 1], 5, axis=0), 0.0) + jnp.where(
                        row8 == 1, pltpu.roll(y[1][part - 1], 6, axis=0), 0.0
                    )
                    r_ref[f, edge_at, :] = p.astype(BF16)

            m0, m1 = halves(m_ref[at, :])
            w = (m0 * tab[12], m1 * tab[13])
            edges(fields, w)

            def pool(v):
                v = v + roll(v, 4)
                return v + roll(v, 7)

            inv = [1.0 / pool(v) for v in w]
            u = halves(x_ref[0, at, :])
            v = halves(x_ref[1, at, :])
            uw = (u[0] * w[0], u[1] * w[1])
            vw = (v[0] * w[0], v[1] * w[1])
            for f in range(fields):
                x = u if f == 0 else v if f == 1 else halves(x_ref[f, at, :])
                r4 = (roll(x[0], 4), roll(x[1], 4))
                out = []
                means = []
                for h in range(2):
                    da = (
                        tab[4 * h] * x[0]
                        + tab[4 * h + 1] * r4[0]
                        + tab[4 * h + 2] * x[1]
                        + tab[4 * h + 3] * r4[1]
                    )
                    db = tab[8] * x[h]
                    for k in (1, 2, 3):
                        turned = jnp.where(sub >= k, roll(x[h], k), roll(r4[h], k))
                        db = db + tab[8 + k] * turned
                    out.append(uw[h] * da + vw[h] * db)
                    means.append(pool(x[h] * w[h]) * inv[h])
                edges(f, out)
                o_ref[f, at, :] = jnp.stack(out, axis=1).reshape(group, 128)
                mean_ref[at, f * 128 : (f + 1) * 128] = (
                    jnp.stack(means, axis=1).reshape(group, 128).astype(BF16)
                )
        return carry

    lax.fori_loop(0, rows // span, step, 0)
    c_ref[...] = jnp.dot(pick_ref[...], mean_ref[...], preferred_element_type=F32).astype(BF16)


def pick_table(group):
    pick = np.zeros((group // 4, group), np.float32)
    for c in range(group // 4):
        element, p, q = c // 4, (c // 2) % 2, c % 2
        pick[c, element * 16 + p * 8 + q * 2] = 1.0
    return pick


def tendencies(x, mass, rows_a):
    fields, rows, levels = x.shape
    span = rows // rows_a
    lot = 3
    block = lot * span
    edge = jax.ShapeDtypeStruct((fields + 1, rows_a * 8, levels), BF16)
    return pl.pallas_call(
        lambda *refs: tend_body(*refs, per=span // 16),
        grid=(rows // block,),
        in_specs=[
            pl.BlockSpec((fields, block, levels), lambda i: (0, i, 0)),
            pl.BlockSpec((block, levels), lambda i: (i, 0)),
            pl.BlockSpec((14, 8, 128), lambda i: (0, 0, 0)),
            pl.BlockSpec((block // 4, block), lambda i: (0, 0)),
        ],
        out_specs=[
            pl.BlockSpec((fields, block, levels), lambda i: (0, i, 0)),
            pl.BlockSpec((block // 4, fields * levels), lambda i: (i, 0)),
            pl.BlockSpec((fields + 1, lot * 8, levels), lambda i: (0, i, 0)),
            pl.BlockSpec((fields + 1, lot * 8, levels), lambda i: (0, i, 0)),
        ],
        out_shape=[
            jax.ShapeDtypeStruct((fields, rows, levels), F32),
            jax.ShapeDtypeStruct((rows // 4, fields * levels), BF16),
            edge,
            edge,
        ],
        scratch_shapes=[pltpu.VMEM((block, fields * levels), BF16)],
        name="tendencies",
        compiler_params=pltpu.CompilerParams(vmem_limit_bytes=60 << 20),
    )(x, mass, jnp.asarray(row_tables()), jnp.asarray(pick_table(block), BF16))


def section_body(
    t_ref, x_ref, m_ref, q_ref, left_ref, right_ref, o_ref, rim_ref, head_ref, tail_ref, inv_ref, *, per
):
    rows = x_ref.shape[1]
    span = per * 16
    count = rows // span
    fields = head_ref.shape[0] - 1
    s = lax.broadcasted_iota(jnp.int32, (per, 8, 128), 1)
    low = s < 4
    first = s % 4 == 0
    last = s % 4 == 3
    f = pl.program_id(0)

    def halves(v):
        v = v.reshape(per, 2, 8, 128)
        return v[:, 0], v[:, 1]

    def window(a):
        return pl.ds(pl.multiple_of(a * span, span), span)

    def across(here, a, k):
        at = pl.ds(pl.multiple_of(a * 8, 8), 8)
        left = left_ref[k, at, :].astype(F32)[None]
        right = right_ref[k, at, :].astype(F32)[None]
        result = []
        for h, p in enumerate(here):
            near = jnp.where(first[:1], left if h == 0 else roll(left, 7), 0.0)
            far = jnp.where(last[:1], roll(right, 3 - h), 0.0)
            up = jnp.where(last, roll(p, 3), 0.0)
            down = jnp.where(first, roll(p, 5), 0.0)
            up = jnp.concatenate([up[1:], far], axis=0)
            down = jnp.concatenate([near, down[:-1]], axis=0)
            result.append(p + up + down)
        return result

    def rims(k, p0, p1):
        rim_ref[k, 0] = p0.reshape(per * 8, 128)
        rim_ref[k, 1] = p1.reshape(per * 8, 128)
        p0 = p0.reshape(per // 2, 2, 8, 128)
        p1 = p1.reshape(per // 2, 2, 8, 128)
        half = low[: per // 2]
        head_ref[k] = (
            jnp.where(half, p0[:, 0], roll(p0[:, 1], 4)).reshape(per * 4, 128).astype(BF16)
        )
        tail_ref[k] = (
            jnp.where(half, roll(p1[:, 0], 4), p1[:, 1]).reshape(per * 4, 128).astype(BF16)
        )

    def sweep(load, k, put0, put1):
        p0, p1 = across(load(0), 0, k)
        start = p0
        put0(0, p0, True)

        def step(a, before):
            p0, p1 = across(load(a), a, k)
            put0(a, p0 + jnp.where(low, roll(before, 4), 0.0), False)
            put1(a - 1, before + jnp.where(low, 0.0, roll(p0, 4)), False)
            return p1

        p1 = lax.fori_loop(1, count, step, p1)
        put1(count - 1, p1, True)
        rims(k, start, p1)

    @pl.when(f == 0)
    def _():
        def mass_at(a):
            m0, m1 = halves(m_ref[window(a), :])
            return m0 * q_ref[0][None], m1 * q_ref[1][None]

        def put(h):
            def run(a, v, rim):
                inv_ref[a, :, h] = jnp.zeros_like(v) if rim else section_step / v
            return run

        sweep(mass_at, fields, put(0), put(1))

    def put(h):
        def run(a, v, rim):
            x = halves(x_ref[0, window(a), :])[h]
            o_ref[0, a, :, h] = x + v * inv_ref[a, :, h]
        return run

    sweep(lambda a: halves(t_ref[0, window(a), :]), f, put(0), put(1))


def section_of(t, x, mass, left, right, rows_a):
    fields, rows, levels = x.shape
    per = rows // rows_a // 16
    whole = lambda a: pl.BlockSpec(a.shape, lambda f: (0,) * a.ndim)
    quad = jnp.asarray(row_tables()[12:14])
    one = pl.BlockSpec((1, rows, levels), lambda f: (f, 0, 0))
    edge = jax.ShapeDtypeStruct((fields + 1, per * 4, levels), BF16)
    rim = jax.ShapeDtypeStruct((fields + 1, 2, per * 8, levels), F32)
    section, rim, head, tail = pl.pallas_call(
        lambda *refs: section_body(*refs, per=per),
        grid=(fields,),
        in_specs=[one, one] + [whole(a) for a in (mass, quad, left, right)],
        out_specs=[
            pl.BlockSpec((1, rows_a, per, 2, 8, levels), lambda f: (f, 0, 0, 0, 0, 0)),
            whole(rim),
            whole(edge),
            whole(edge),
        ],
        out_shape=[
            jax.ShapeDtypeStruct((fields, rows_a, per, 2, 8, levels), F32),
            rim,
            edge,
            edge,
        ],
        scratch_shapes=[pltpu.VMEM((rows_a, per, 2, 8, levels), F32)],
        name="section",
        compiler_params=pltpu.CompilerParams(vmem_limit_bytes=60 << 20),
    )(t, x, mass, quad, left, right)
    return section.reshape(fields, rows, levels), rim, head, tail


def places_body(owner_ref, o_ref, *, devices, capacity):
    cols = owner_ref.shape[0]
    owner = owner_ref[...]
    hits = owner == lax.broadcasted_iota(jnp.int32, (cols, devices), 1)
    hits = jnp.where(hits, 1.0, 0.0)
    before = lax.broadcasted_iota(jnp.int32, (cols, cols), 0) > lax.broadcasted_iota(
        jnp.int32, (cols, cols), 1
    )
    before = jnp.where(before, 1.0, 0.0).astype(BF16)
    earlier = jnp.dot(before, hits.astype(BF16), preferred_element_type=F32)
    slot = jnp.sum(hits * earlier, axis=1, keepdims=True).astype(jnp.int32)
    place = owner * capacity + slot
    wide = lax.broadcasted_iota(jnp.int32, (cols, devices * capacity), 1)
    o_ref[...] = jnp.where(place == wide, 1.0, 0.0).astype(BF16)


def places(owner, devices, capacity):
    return pl.pallas_call(
        lambda a, o: places_body(a, o, devices=devices, capacity=capacity),
        out_shape=jax.ShapeDtypeStruct((owner.shape[0], devices * capacity), BF16),
        name="places",
        compiler_params=pltpu.CompilerParams(vmem_limit_bytes=60 << 20),
    )(owner)


def first_body(s_ref, w_ref, b_ref, o_ref, w2_ref):
    width = s_ref.shape[1]
    rest = w_ref.shape[0] - width
    o_ref[...] = jnp.dot(s_ref[...], w_ref[:width, :], preferred_element_type=F32) + b_ref[...]
    w2_ref[:rest, :] = w_ref[width:, :]
    w2_ref[rest:, :] = jnp.zeros((w2_ref.shape[0] - rest, w2_ref.shape[1]), BF16)


def first_part(state, weight, bias, padded):
    cols = state.shape[0]
    hidden = weight.shape[1]
    return pl.pallas_call(
        first_body,
        out_shape=[jax.ShapeDtypeStruct((cols, hidden), F32), jax.ShapeDtypeStruct((padded, hidden), BF16)],
        name="first_part",
        compiler_params=pltpu.CompilerParams(vmem_limit_bytes=60 << 20),
    )(state, weight, bias)


def finish_body(
    sel_ref, aux_ref, w_ref, part_ref, wo_ref, bo_ref, spread_ref, x_ref, rim_ref, above_ref, below_ref, o_ref
):
    fields = x_ref.shape[0]
    levels = x_ref.shape[2]
    block = x_ref.shape[1] // 4
    i = pl.program_id(0)
    at = pl.ds(pl.multiple_of(i * block, block), block)
    aux = jnp.dot(sel_ref[at, :], aux_ref[...], preferred_element_type=F32).astype(BF16)
    v = part_ref[at, :] + jnp.dot(aux, w_ref[...], preferred_element_type=F32)
    hidden = (v / (1.0 + jnp.exp(-v))).astype(BF16)
    inc = jnp.dot(hidden, wo_ref[...], preferred_element_type=F32) + bo_ref[...]
    inc = inc.astype(BF16)
    group = spread_ref.shape[1]
    for g in range(block // group):
        wide = jnp.dot(
            spread_ref[...], inc[g * group : (g + 1) * group], preferred_element_type=F32
        )
        to = pl.ds(g * group * 4, group * 4)
        for f in range(fields):
            o_ref[f, to, :] = x_ref[f, to, :] + wide[:, f * levels : (f + 1) * levels]

    per = rim_ref.shape[2] // 8
    low = lax.broadcasted_iota(jnp.int32, (per // 2, 8, 128), 1) < 4

    def patch(h, halo, start):
        def total(k):
            p = halo[k].astype(F32).reshape(per // 2, 8, 128)
            q = roll(p, 4)
            if h == 0:
                add = jnp.stack([jnp.where(low, p, 0.0), jnp.where(low, q, 0.0)], axis=1)
            else:
                add = jnp.stack([jnp.where(low, 0.0, q), jnp.where(low, 0.0, p)], axis=1)
            return rim_ref[k, h].reshape(per, 8, 128) + add.reshape(per, 8, 128)

        scale = section_step / total(fields)
        to = pl.ds(start, per * 16)
        for f in range(fields):
            gain = total(f) * scale
            none = jnp.zeros_like(gain)
            both = jnp.stack([gain, none] if h == 0 else [none, gain], axis=1)
            o_ref[f, to, :] = o_ref[f, to, :] + both.reshape(per * 16, 128)

    @pl.when(i == 0)
    def _():
        patch(0, above_ref, 0)

    @pl.when(i == pl.num_programs(0) - 1)
    def _():
        patch(1, below_ref, block * 4 - per * 16)


def spread_table(group):
    spread = np.zeros((group * 4, group), np.float32)
    for r in range(group * 4):
        e, i, j = r // 16, (r // 4) % 4, r % 4
        spread[r, e * 4 + (i // 2) * 2 + j // 2] = 1.0
    return spread


def finish(sel, aux, weight, part, weight_out, bias_out, x, rim, above, below):
    cols = sel.shape[0]
    fields, rows, levels = x.shape
    block = 256
    spread = jnp.asarray(spread_table(128), BF16)
    full = lambda a: pl.BlockSpec(a.shape, lambda i: (0,) * a.ndim)
    moving = pl.BlockSpec((fields, block * 4, levels), lambda i: (0, i, 0))
    before = (sel, aux, weight, part, weight_out, bias_out, spread)
    after = (rim, above, below)
    return pl.pallas_call(
        finish_body,
        grid=(cols // block,),
        in_specs=[full(a) for a in before] + [moving] + [full(a) for a in after],
        out_specs=moving,
        out_shape=jax.ShapeDtypeStruct(x.shape, F32),
        name="finish",
        compiler_params=pltpu.CompilerParams(vmem_limit_bytes=60 << 20),
    )(*before, x, *after)


def shards(
    prognostic, layer_mass, column_aux, group_owner, weight_in, bias_in, weight_out, bias_out
):
    fields, rows_a, rows_b, _, _, levels = prognostic.shape
    n_curve, n_sub = lax.axis_size("curve"), lax.axis_size("sub")
    devices = n_curve * n_sub
    capacity = column_aux.shape[0] // devices
    aux_width = column_aux.shape[1]
    padded = -(-aux_width // 128) * 128
    rows = rows_a * rows_b * 16

    home = turn(column_aux.T, padded).reshape(devices, capacity, padded)
    home = lax.all_to_all(home, AXES, split_axis=0, concat_axis=0, tiled=True)
    home = home.reshape(devices * capacity, padded)

    x = prognostic.reshape(fields, rows, levels)
    mass = layer_mass.reshape(rows, levels)
    tend, state, left_out, right_out = tendencies(x, mass, rows_a)

    def ahead(n):
        return [(i, (i + 1) % n) for i in range(n)]

    def back(n):
        return [((i + 1) % n, i) for i in range(n)]

    left = lax.ppermute(right_out, "sub", ahead(n_sub))
    right = lax.ppermute(left_out, "sub", back(n_sub))
    section, rim, head, tail = section_of(tend, x, mass, left, right, rows_a)
    above = lax.ppermute(tail, "curve", ahead(n_curve))
    below = lax.ppermute(head, "curve", back(n_curve))

    sel = places(group_owner, devices, capacity)
    part, weight_aux = first_part(state, weight_in, bias_in[None], padded)
    out = finish(sel, home, weight_aux, part, weight_out, bias_out[None], section, rim, above, below)
    return out.reshape(prognostic.shape)


def solution(mesh):
    return jax.shard_map(
        shards,
        mesh=mesh,
        in_specs=(
            P(None, "curve", "sub", None, None, None),
            P("curve", "sub", None, None, None),
            P(("curve", "sub"), None),
            P(("curve", "sub"), None),
            P(),
            P(),
            P(),
            P(),
        ),
        out_specs=P(None, "curve", "sub", None, None, None),
        check_vma=False,
    )
```

```python
import jax
import jax.numpy as jnp
import numpy as np
from jax import lax
from jax.experimental import pallas as pl
from jax.experimental.pallas import tpu as pltpu
from jax.sharding import PartitionSpec as P

section_step = 0.1
AXES = ("curve", "sub")
F32 = jnp.float32
BF16 = jnp.bfloat16


def node_tables():
    nodes = np.array([-1.0, -1.0 / np.sqrt(5.0), 1.0 / np.sqrt(5.0), 1.0])
    quadrature = np.array([1.0 / 6.0, 5.0 / 6.0, 5.0 / 6.0, 1.0 / 6.0])
    products = np.array(
        [np.prod([nodes[i] - nodes[k] for k in range(4) if k != i]) for i in range(4)]
    )
    derivative = np.zeros((4, 4))
    for i in range(4):
        for k in range(4):
            if i != k:
                derivative[i, k] = products[i] / (products[k] * (nodes[i] - nodes[k]))
            else:
                derivative[i, i] = sum(1.0 / (nodes[i] - nodes[m]) for m in range(4) if m != i)
    return derivative.astype(np.float32), quadrature.astype(np.float32)


def row_tables():
    d, w = node_tables()
    s = np.arange(8)
    i, j = s // 4, s % 4
    tables = []
    for half in (0, 2):
        for column in (i, 1 - i, 2 + i, 3 - i):
            tables.append(-d[half + i, column])
    for shift in range(4):
        tables.append(-d[j, (j - shift) % 4])
    for half in (0, 2):
        tables.append(w[half + i] * w[j])
    return np.repeat(np.stack(tables)[:, :, None], 128, axis=2).astype(np.float32)


def lane_rows(x):
    return lax.broadcasted_iota(jnp.int32, x, len(x) - 2)


def roll(x, shift):
    return pltpu.roll(x, shift % 8, axis=1)


def turn_body(x_ref, o_ref):
    width = x_ref.shape[0]
    o_ref[:, :width] = x_ref[...].T
    o_ref[:, width:] = jnp.zeros((o_ref.shape[0], o_ref.shape[1] - width), BF16)


def turn(aux_t, padded):
    width, rows = aux_t.shape
    block = rows // 2
    return pl.pallas_call(
        turn_body,
        grid=(rows // block,),
        in_specs=[pl.BlockSpec((width, block), lambda i: (0, i))],
        out_specs=pl.BlockSpec((block, padded), lambda i: (i, 0)),
        out_shape=jax.ShapeDtypeStruct((rows, padded), BF16),
        name="turn",
        compiler_params=pltpu.CompilerParams(vmem_limit_bytes=56 << 20),
    )(aux_t)


def tend_body(x_ref, m_ref, q_ref, deriv_ref, pick_ref, o_ref, c_ref, l_ref, r_ref):
    fields, rows, levels = x_ref.shape
    group = q_ref.shape[0]
    cells = group // 4
    lines = (pick_ref.shape[0] - cells) // 2

    for g in range(rows // group):
        at = pl.ds(g * group, group)
        cell_at = pl.ds(g * cells, cells)
        line_at = pl.ds(g * lines, lines)

        def picked(first, second):
            y = jnp.dot(
                pick_ref[...], jnp.concatenate([first, second], axis=1), preferred_element_type=F32
            )
            return y[:cells, :levels], y[cells:, levels:].astype(BF16)

        w = m_ref[at, :] * q_ref[...]
        wb = w.astype(BF16)
        mass, edge = picked(wb, wb)
        inv = 1.0 / mass
        l_ref[fields, line_at, :] = edge[:lines]
        r_ref[fields, line_at, :] = edge[lines:]
        uw = x_ref[0, at, :] * w
        vw = x_ref[1, at, :] * w
        for pair in range(0, fields, 2):
            both = (x_ref[pair, at, :], x_ref[pair + 1, at, :])
            d = jnp.dot(
                deriv_ref[...],
                jnp.concatenate([x.astype(BF16) for x in both], axis=1),
                preferred_element_type=F32,
            )
            for k, x in enumerate(both):
                f = pair + k
                lanes = slice(k * levels, (k + 1) * levels)
                out = (uw * d[:group, lanes] + vw * d[group:, lanes]).astype(BF16)
                xw = (uw if f == 0 else vw if f == 1 else x * w).astype(BF16)
                o_ref[f, at, :] = out
                mean, edge = picked(xw, out)
                c_ref[cell_at, f * levels : (f + 1) * levels] = (mean * inv).astype(BF16)
                l_ref[f, line_at, :] = edge[:lines]
                r_ref[f, line_at, :] = edge[lines:]


def derivative_table(group):
    d = node_tables()[0]
    r = np.arange(group)
    same = (r[:, None] // 16) == (r[None, :] // 16)
    i, j = (r // 4) % 4, r % 4
    along_first = np.where(same & (j[:, None] == j[None, :]), d[i[:, None], i[None, :]], 0.0)
    along_second = np.where(same & (i[:, None] == i[None, :]), d[j[:, None], j[None, :]], 0.0)
    return -np.concatenate([along_first, along_second], axis=0)


def pick_table(group, span):
    r = np.arange(group)
    cells = np.zeros((group // 4, group), np.float32)
    cells[(r // 16) * 4 + ((r // 8) % 2) * 2 + (r % 4) // 2, r] = 1.0
    lines = [np.zeros((group // span * 8, group), np.float32) for _ in range(2)]
    for a in range(group // span):
        for i in range(4):
            to = a * 8 + (i % 2) * 4 + i // 2
            lines[0][to, a * span + i * 4] = 1.0
            lines[1][to, (a + 1) * span - 16 + i * 4 + 3] = 1.0
    return np.concatenate([cells] + lines, axis=0)


def tendencies(x, mass, rows_a):
    fields, rows, levels = x.shape
    span = rows // rows_a
    group = 2 * span
    lot = 4
    block = lot * span
    quad = np.tile(row_tables()[12:14].reshape(16, 128), (group // 16, 1))
    deriv = jnp.asarray(derivative_table(group), BF16)
    pick = jnp.asarray(pick_table(group, span), BF16)
    edge = jax.ShapeDtypeStruct((fields + 1, rows_a * 8, levels), BF16)
    whole = lambda a: pl.BlockSpec(a.shape, lambda i: (0, 0))
    return pl.pallas_call(
        tend_body,
        grid=(rows // block,),
        in_specs=[
            pl.BlockSpec((fields, block, levels), lambda i: (0, i, 0)),
            pl.BlockSpec((block, levels), lambda i: (i, 0)),
            whole(quad),
            whole(deriv),
            whole(pick),
        ],
        out_specs=[
            pl.BlockSpec((fields, block, levels), lambda i: (0, i, 0)),
            pl.BlockSpec((block // 4, fields * levels), lambda i: (i, 0)),
            pl.BlockSpec((fields + 1, lot * 8, levels), lambda i: (0, i, 0)),
            pl.BlockSpec((fields + 1, lot * 8, levels), lambda i: (0, i, 0)),
        ],
        out_shape=[
            jax.ShapeDtypeStruct((fields, rows, levels), BF16),
            jax.ShapeDtypeStruct((rows // 4, fields * levels), BF16),
            edge,
            edge,
        ],
        name="tendencies",
        compiler_params=pltpu.CompilerParams(vmem_limit_bytes=56 << 20),
    )(x, mass, jnp.asarray(quad), deriv, pick)


def section_body(
    t_ref, x_ref, m_ref, q_ref, left_ref, right_ref, o_ref, rim_ref, head_ref, tail_ref, inv_ref, *, per
):
    rows = x_ref.shape[1]
    span = per * 16
    count = rows // span
    fields = head_ref.shape[0] - 1
    s = lax.broadcasted_iota(jnp.int32, (per, 8, 128), 1)
    low = s < 4
    first = s % 4 == 0
    last = s % 4 == 3
    f = pl.program_id(0)

    def halves(v):
        v = v.reshape(per, 2, 8, 128)
        return v[:, 0], v[:, 1]

    def window(a):
        return pl.ds(pl.multiple_of(a * span, span), span)

    def across(here, a, k):
        at = pl.ds(pl.multiple_of(a * 8, 8), 8)
        left = left_ref[k, at, :].astype(F32)[None]
        right = right_ref[k, at, :].astype(F32)[None]
        result = []
        for h, p in enumerate(here):
            near = jnp.where(first[:1], left if h == 0 else roll(left, 7), 0.0)
            far = jnp.where(last[:1], roll(right, 3 - h), 0.0)
            up = jnp.where(last, roll(p, 3), 0.0)
            down = jnp.where(first, roll(p, 5), 0.0)
            up = jnp.concatenate([up[1:], far], axis=0)
            down = jnp.concatenate([near, down[:-1]], axis=0)
            result.append(p + up + down)
        return result

    def rims(k, p0, p1):
        rim_ref[k, 0] = p0.reshape(per * 8, 128)
        rim_ref[k, 1] = p1.reshape(per * 8, 128)
        p0 = p0.reshape(per // 2, 2, 8, 128)
        p1 = p1.reshape(per // 2, 2, 8, 128)
        half = low[: per // 2]
        head_ref[k] = (
            jnp.where(half, p0[:, 0], roll(p0[:, 1], 4)).reshape(per * 4, 128).astype(BF16)
        )
        tail_ref[k] = (
            jnp.where(half, roll(p1[:, 0], 4), p1[:, 1]).reshape(per * 4, 128).astype(BF16)
        )

    def sweep(load, k, put):
        start, p1 = across(load(0), 0, k)

        def step(a, carry):
            y0, before = carry
            p0, p1 = across(load(a), a, k)
            put(a - 1, y0, before + jnp.where(low, 0.0, roll(p0, 4)))
            return p0 + jnp.where(low, roll(before, 4), 0.0), p1

        y0, p1 = lax.fori_loop(1, count, step, (start, p1))
        put(count - 1, y0, p1)
        rims(k, start, p1)

    def joined(y0, y1):
        return jnp.stack([y0, y1], axis=1).reshape(span, 128)

    @pl.when(f == 0)
    def _():
        def mass_at(a):
            m0, m1 = halves(m_ref[window(a), :])
            return m0 * q_ref[0][None], m1 * q_ref[1][None]

        def put(a, y0, y1):
            inv_ref[window(a), :] = section_step / joined(y0, y1)

        sweep(mass_at, fields, put)
        top = pl.ds(0, span)
        v0, v1 = halves(inv_ref[top, :])
        inv_ref[top, :] = joined(jnp.zeros_like(v0), v1)
        end = pl.ds(rows - span, span)
        v0, v1 = halves(inv_ref[end, :])
        inv_ref[end, :] = joined(v0, jnp.zeros_like(v1))

    def put(a, y0, y1):
        y = x_ref[0, window(a), :] + joined(y0, y1) * inv_ref[window(a), :]
        o_ref[0, window(a), :] = y.astype(o_ref.dtype)

    sweep(lambda a: halves(t_ref[0, window(a), :].astype(F32)), f, put)


def section_of(t, x, mass, left, right, rows_a):
    fields, rows, levels = x.shape
    per = rows // rows_a // 16
    whole = lambda a: pl.BlockSpec(a.shape, lambda f: (0,) * a.ndim)
    quad = jnp.asarray(row_tables()[12:14])
    one = pl.BlockSpec((1, rows, levels), lambda f: (f, 0, 0))
    edge = jax.ShapeDtypeStruct((fields + 1, per * 4, levels), BF16)
    rim = jax.ShapeDtypeStruct((fields + 1, 2, per * 8, levels), F32)
    section, rim, head, tail = pl.pallas_call(
        lambda *refs: section_body(*refs, per=per),
        grid=(fields,),
        in_specs=[one, one] + [whole(a) for a in (mass, quad, left, right)],
        out_specs=[
            one,
            whole(rim),
            whole(edge),
            whole(edge),
        ],
        out_shape=[
            jax.ShapeDtypeStruct(x.shape, BF16),
            rim,
            edge,
            edge,
        ],
        scratch_shapes=[pltpu.VMEM((rows, levels), F32)],
        name="section",
        compiler_params=pltpu.CompilerParams(vmem_limit_bytes=56 << 20),
    )(t, x, mass, quad, left, right)
    return section, rim, head, tail


def places_body(owner_ref, o_ref, *, devices, capacity):
    cols = owner_ref.shape[0]
    owner = owner_ref[...]
    hits = owner == lax.broadcasted_iota(jnp.int32, (cols, devices), 1)
    hits = jnp.where(hits, 1.0, 0.0)
    before = lax.broadcasted_iota(jnp.int32, (cols, cols), 0) > lax.broadcasted_iota(
        jnp.int32, (cols, cols), 1
    )
    before = jnp.where(before, 1.0, 0.0).astype(BF16)
    earlier = jnp.dot(before, hits.astype(BF16), preferred_element_type=F32)
    slot = jnp.sum(hits * earlier, axis=1, keepdims=True).astype(jnp.int32)
    place = owner * capacity + slot
    wide = lax.broadcasted_iota(jnp.int32, (cols, devices * capacity), 1)
    o_ref[...] = jnp.where(place == wide, 1.0, 0.0).astype(BF16)


def places(owner, devices, capacity):
    return pl.pallas_call(
        lambda a, o: places_body(a, o, devices=devices, capacity=capacity),
        out_shape=jax.ShapeDtypeStruct((owner.shape[0], devices * capacity), BF16),
        name="places",
        compiler_params=pltpu.CompilerParams(vmem_limit_bytes=56 << 20),
    )(owner)


def first_body(s_ref, w_ref, b_ref, o_ref, w2_ref):
    width = s_ref.shape[1]
    rest = w_ref.shape[0] - width
    y = jnp.dot(s_ref[...], w_ref[:width, :], preferred_element_type=F32) + b_ref[...]
    o_ref[...] = y.astype(BF16)
    w2_ref[:rest, :] = w_ref[width:, :]
    w2_ref[rest:, :] = jnp.zeros((w2_ref.shape[0] - rest, w2_ref.shape[1]), BF16)


def first_part(state, weight, bias, padded):
    cols, width = state.shape
    depth, hidden = weight.shape
    block = 512
    return pl.pallas_call(
        first_body,
        grid=(hidden // block,),
        in_specs=[
            pl.BlockSpec((cols, width), lambda i: (0, 0)),
            pl.BlockSpec((depth, block), lambda i: (0, i)),
            pl.BlockSpec((1, block), lambda i: (0, i)),
        ],
        out_specs=[
            pl.BlockSpec((cols, block), lambda i: (0, i)),
            pl.BlockSpec((padded, block), lambda i: (0, i)),
        ],
        out_shape=[
            jax.ShapeDtypeStruct((cols, hidden), BF16),
            jax.ShapeDtypeStruct((padded, hidden), BF16),
        ],
        name="first_part",
        compiler_params=pltpu.CompilerParams(vmem_limit_bytes=56 << 20),
    )(state, weight, bias)


def finish_body(
    sel_hbm, w_hbm, part_hbm, wo_hbm, x_hbm, home_ref, bo_ref, spread_ref, rim_ref, above_ref, below_ref, out_hbm,
    sel_ref, w_ref, part_ref, wo_ref, x_ref, aux_ref, o_ref, sem, out_sem, *, block
):
    fields, rows, levels = x_ref.shape
    cols = sel_ref.shape[0]
    steps = cols // block

    copies = {}

    def fetch(name, src, dst):
        copies[name] = pltpu.make_async_copy(src, dst, sem.at[len(copies)])
        copies[name].start()

    def rows_of(k, scale=1):
        return pl.ds(k * block * scale, block * scale)

    fetch("sel", sel_hbm, sel_ref)
    fetch("w", w_hbm, w_ref)
    fetch("part0", part_hbm.at[rows_of(0), :], part_ref.at[rows_of(0), :])
    fetch("wo", wo_hbm, wo_ref)
    fetch("x0", x_hbm.at[:, rows_of(0, 4), :], x_ref.at[:, rows_of(0, 4), :])
    for k in range(1, steps):
        fetch(f"part{k}", part_hbm.at[rows_of(k), :], part_ref.at[rows_of(k), :])
        fetch(f"x{k}", x_hbm.at[:, rows_of(k, 4), :], x_ref.at[:, rows_of(k, 4), :])

    per = rim_ref.shape[2] // 8
    low = lax.broadcasted_iota(jnp.int32, (per // 2, 8, 128), 1) < 4

    def patch(h, halo, start):
        def total(k):
            p = halo[k].astype(F32).reshape(per // 2, 8, 128)
            q = roll(p, 4)
            if h == 0:
                add = jnp.stack([jnp.where(low, p, 0.0), jnp.where(low, q, 0.0)], axis=1)
            else:
                add = jnp.stack([jnp.where(low, 0.0, q), jnp.where(low, 0.0, p)], axis=1)
            return rim_ref[k, h].reshape(per, 8, 128) + add.reshape(per, 8, 128)

        scale = section_step / total(fields)
        to = pl.ds(start, per * 16)
        for f in range(fields):
            gain = total(f) * scale
            none = jnp.zeros_like(gain)
            both = jnp.stack([gain, none] if h == 0 else [none, gain], axis=1)
            o_ref[f, to, :] = o_ref[f, to, :] + both.reshape(per * 16, 128)

    copies["sel"].wait()
    aux_ref[...] = jnp.dot(sel_ref[...], home_ref[...], preferred_element_type=F32).astype(BF16)
    copies["w"].wait()
    group = spread_ref.shape[1]
    outs = []
    for k in range(steps):
        at = rows_of(k)
        copies[f"part{k}"].wait()
        v = part_ref[at, :].astype(F32) + jnp.dot(aux_ref[at, :], w_ref[...], preferred_element_type=F32)
        half = 0.5 * v
        hidden = (half + half * jnp.tanh(half)).astype(BF16)
        if k == 0:
            copies["wo"].wait()
        inc = jnp.dot(hidden, wo_ref[...], preferred_element_type=F32) + bo_ref[...]
        inc = inc.astype(BF16)
        copies[f"x{k}"].wait()
        for g in range(block // group):
            wide = jnp.dot(
                spread_ref[...], inc[g * group : (g + 1) * group], preferred_element_type=F32
            )
            to = pl.ds((k * block + g * group) * 4, group * 4)
            for f in range(fields):
                o_ref[f, to, :] = x_ref[f, to, :].astype(F32) + wide[:, f * levels : (f + 1) * levels]
        if k == 0:
            patch(0, above_ref, 0)
        if k == steps - 1:
            patch(1, below_ref, rows - per * 16)
        done = pltpu.make_async_copy(
            o_ref.at[:, rows_of(k, 4), :], out_hbm.at[:, rows_of(k, 4), :], out_sem.at[k]
        )
        done.start()
        outs.append(done)
    for done in outs:
        done.wait()


def spread_table(group):
    spread = np.zeros((group * 4, group), np.float32)
    for r in range(group * 4):
        e, i, j = r // 16, (r // 4) % 4, r % 4
        spread[r, e * 4 + (i // 2) * 2 + j // 2] = 1.0
    return spread


def finish(sel, home, weight, part, weight_out, bias_out, x, rim, above, below):
    cols = sel.shape[0]
    fields, rows, levels = x.shape
    block = 256
    steps = cols // block
    spread = jnp.asarray(spread_table(128), BF16)
    far = pl.BlockSpec(memory_space=pltpu.HBM)
    full = lambda a: pl.BlockSpec(a.shape, lambda: (0,) * a.ndim)
    large = (sel, weight, part, weight_out, x)
    small = (home, bias_out, spread, rim, above, below)
    return pl.pallas_call(
        lambda *refs: finish_body(*refs, block=block),
        in_specs=[far] * len(large)
        + [pl.BlockSpec(memory_space=pltpu.VMEM)]
        + [full(a) for a in small[1:]],
        out_specs=far,
        out_shape=jax.ShapeDtypeStruct(x.shape, F32),
        scratch_shapes=[pltpu.VMEM(a.shape, a.dtype) for a in large]
        + [
            pltpu.VMEM((cols, home.shape[1]), BF16),
            pltpu.VMEM(x.shape, F32),
            pltpu.SemaphoreType.DMA((3 + 2 * steps,)),
            pltpu.SemaphoreType.DMA((steps,)),
        ],
        name="finish",
        compiler_params=pltpu.CompilerParams(vmem_limit_bytes=50 << 20),
    )(*large, *small)


def shards(
    prognostic, layer_mass, column_aux, group_owner, weight_in, bias_in, weight_out, bias_out
):
    fields, rows_a, rows_b, _, _, levels = prognostic.shape
    n_curve, n_sub = lax.axis_size("curve"), lax.axis_size("sub")
    devices = n_curve * n_sub
    capacity = column_aux.shape[0] // devices
    aux_width = column_aux.shape[1]
    padded = -(-aux_width // 128) * 128
    rows = rows_a * rows_b * 16

    home = turn(column_aux.T, padded).reshape(devices, capacity, padded)
    home = lax.all_to_all(home, AXES, split_axis=0, concat_axis=0, tiled=True)
    home = home.reshape(devices * capacity, padded)

    x = prognostic.reshape(fields, rows, levels)
    mass = layer_mass.reshape(rows, levels)
    tend, state, left_out, right_out = tendencies(x, mass, rows_a)

    def ahead(n):
        return [(i, (i + 1) % n) for i in range(n)]

    def back(n):
        return [((i + 1) % n, i) for i in range(n)]

    left = lax.ppermute(right_out, "sub", ahead(n_sub))
    right = lax.ppermute(left_out, "sub", back(n_sub))
    section, rim, head, tail = section_of(tend, x, mass, left, right, rows_a)
    above = lax.ppermute(tail, "curve", ahead(n_curve))
    below = lax.ppermute(head, "curve", back(n_curve))

    sel = places(group_owner, devices, capacity)
    part, weight_aux = first_part(state, weight_in, bias_in[None], padded)
    out = finish(sel, home, weight_aux, part, weight_out, bias_out[None], section, rim, above, below)
    return out.reshape(prognostic.shape)


def solution(mesh):
    return jax.shard_map(
        shards,
        mesh=mesh,
        in_specs=(
            P(None, "curve", "sub", None, None, None),
            P("curve", "sub", None, None, None),
            P(("curve", "sub"), None),
            P(("curve", "sub"), None),
            P(),
            P(),
            P(),
            P(),
        ),
        out_specs=P(None, "curve", "sub", None, None, None),
        check_vma=False,
    )
```

```python
import jax
import jax.numpy as jnp
import numpy as np
from jax import lax
from jax.experimental import pallas as pl
from jax.experimental.pallas import tpu as pltpu
from jax.sharding import PartitionSpec as P

section_step = 0.1
AXES = ("curve", "sub")
F32 = jnp.float32
BF16 = jnp.bfloat16


def node_tables():
    nodes = np.array([-1.0, -1.0 / np.sqrt(5.0), 1.0 / np.sqrt(5.0), 1.0])
    quadrature = np.array([1.0 / 6.0, 5.0 / 6.0, 5.0 / 6.0, 1.0 / 6.0])
    products = np.array(
        [np.prod([nodes[i] - nodes[k] for k in range(4) if k != i]) for i in range(4)]
    )
    derivative = np.zeros((4, 4))
    for i in range(4):
        for k in range(4):
            if i != k:
                derivative[i, k] = products[i] / (products[k] * (nodes[i] - nodes[k]))
            else:
                derivative[i, i] = sum(1.0 / (nodes[i] - nodes[m]) for m in range(4) if m != i)
    return derivative.astype(np.float32), quadrature.astype(np.float32)


def row_tables():
    d, w = node_tables()
    s = np.arange(8)
    i, j = s // 4, s % 4
    tables = []
    for half in (0, 2):
        for column in (i, 1 - i, 2 + i, 3 - i):
            tables.append(-d[half + i, column])
    for shift in range(4):
        tables.append(-d[j, (j - shift) % 4])
    for half in (0, 2):
        tables.append(w[half + i] * w[j])
    return np.repeat(np.stack(tables)[:, :, None], 128, axis=2).astype(np.float32)


def lane_rows(x):
    return lax.broadcasted_iota(jnp.int32, x, len(x) - 2)


def roll(x, shift):
    return pltpu.roll(x, shift % 8, axis=1)


def turn_body(x_ref, o_ref):
    width = x_ref.shape[0]
    o_ref[:, :width] = x_ref[...].T
    o_ref[:, width:] = jnp.zeros((o_ref.shape[0], o_ref.shape[1] - width), BF16)


def turn(aux_t, padded):
    width, rows = aux_t.shape
    block = rows // 2
    return pl.pallas_call(
        turn_body,
        grid=(rows // block,),
        in_specs=[pl.BlockSpec((width, block), lambda i: (0, i))],
        out_specs=pl.BlockSpec((block, padded), lambda i: (i, 0)),
        out_shape=jax.ShapeDtypeStruct((rows, padded), BF16),
        name="turn",
        compiler_params=pltpu.CompilerParams(vmem_limit_bytes=56 << 20),
    )(aux_t)


def tend_body(x_ref, m_ref, q_ref, deriv_ref, pick_ref, o_ref, c_ref, l_ref, r_ref):
    fields, rows, levels = x_ref.shape
    group = q_ref.shape[0]
    cells = group // 4
    lines = (pick_ref.shape[0] - cells) // 2

    for g in range(rows // group):
        at = pl.ds(g * group, group)
        cell_at = pl.ds(g * cells, cells)
        line_at = pl.ds(g * lines, lines)

        def picked(first, second):
            y = jnp.dot(
                pick_ref[...], jnp.concatenate([first, second], axis=1), preferred_element_type=F32
            )
            return y[:cells, :levels], y[cells:, levels:].astype(BF16)

        w = m_ref[at, :] * q_ref[...]
        wb = w.astype(BF16)
        mass, edge = picked(wb, wb)
        inv = 1.0 / mass
        l_ref[fields, line_at, :] = edge[:lines]
        r_ref[fields, line_at, :] = edge[lines:]
        uw = x_ref[0, at, :] * w
        vw = x_ref[1, at, :] * w
        for pair in range(0, fields, 2):
            both = (x_ref[pair, at, :], x_ref[pair + 1, at, :])
            high = jnp.concatenate([x.astype(BF16) for x in both], axis=1)
            low = jnp.concatenate([(x - x.astype(BF16).astype(F32)).astype(BF16) for x in both], axis=1)
            d = jnp.dot(
                deriv_ref[...], jnp.concatenate([high, high, low], axis=0), preferred_element_type=F32
            )
            for k, x in enumerate(both):
                f = pair + k
                lanes = slice(k * levels, (k + 1) * levels)
                out = (uw * d[:group, lanes] + vw * d[group:, lanes]).astype(BF16)
                xw = (uw if f == 0 else vw if f == 1 else x * w).astype(BF16)
                o_ref[f, at, :] = out
                mean, edge = picked(xw, out)
                c_ref[cell_at, f * levels : (f + 1) * levels] = (mean * inv).astype(BF16)
                l_ref[f, line_at, :] = edge[:lines]
                r_ref[f, line_at, :] = edge[lines:]


def derivative_table(group):
    d = node_tables()[0]
    r = np.arange(group)
    same = (r[:, None] // 16) == (r[None, :] // 16)
    i, j = (r // 4) % 4, r % 4
    along_first = np.where(same & (j[:, None] == j[None, :]), d[i[:, None], i[None, :]], 0.0)
    along_second = np.where(same & (i[:, None] == i[None, :]), d[j[:, None], j[None, :]], 0.0)
    return -np.concatenate([along_first, along_second], axis=0)


def pick_table(group, span):
    r = np.arange(group)
    cells = np.zeros((group // 4, group), np.float32)
    cells[(r // 16) * 4 + ((r // 8) % 2) * 2 + (r % 4) // 2, r] = 1.0
    lines = [np.zeros((group // span * 8, group), np.float32) for _ in range(2)]
    for a in range(group // span):
        for i in range(4):
            to = a * 8 + (i % 2) * 4 + i // 2
            lines[0][to, a * span + i * 4] = 1.0
            lines[1][to, (a + 1) * span - 16 + i * 4 + 3] = 1.0
    return np.concatenate([cells] + lines, axis=0)


def tendencies(x, mass, rows_a):
    fields, rows, levels = x.shape
    span = rows // rows_a
    group = 2 * span
    lot = 4
    block = lot * span
    quad = np.tile(row_tables()[12:14].reshape(16, 128), (group // 16, 1))
    deriv = derivative_table(group)
    top = deriv.astype(jnp.bfloat16)
    deriv = jnp.asarray(np.concatenate([top, (deriv - top.astype(np.float64)).astype(jnp.bfloat16), top], axis=1))
    pick = jnp.asarray(pick_table(group, span), BF16)
    edge = jax.ShapeDtypeStruct((fields + 1, rows_a * 8, levels), BF16)
    whole = lambda a: pl.BlockSpec(a.shape, lambda i: (0, 0))
    return pl.pallas_call(
        tend_body,
        grid=(rows // block,),
        in_specs=[
            pl.BlockSpec((fields, block, levels), lambda i: (0, i, 0)),
            pl.BlockSpec((block, levels), lambda i: (i, 0)),
            whole(quad),
            whole(deriv),
            whole(pick),
        ],
        out_specs=[
            pl.BlockSpec((fields, block, levels), lambda i: (0, i, 0)),
            pl.BlockSpec((block // 4, fields * levels), lambda i: (i, 0)),
            pl.BlockSpec((fields + 1, lot * 8, levels), lambda i: (0, i, 0)),
            pl.BlockSpec((fields + 1, lot * 8, levels), lambda i: (0, i, 0)),
        ],
        out_shape=[
            jax.ShapeDtypeStruct((fields, rows, levels), BF16),
            jax.ShapeDtypeStruct((rows // 4, fields * levels), BF16),
            edge,
            edge,
        ],
        name="tendencies",
        compiler_params=pltpu.CompilerParams(vmem_limit_bytes=56 << 20),
    )(x, mass, jnp.asarray(quad), deriv, pick)


def section_body(
    t_ref, x_ref, m_ref, q_ref, left_ref, right_ref, o_ref, rim_ref, head_ref, tail_ref, inv_ref, *, per
):
    rows = x_ref.shape[1]
    span = per * 16
    count = rows // span
    fields = head_ref.shape[0] - 1
    s = lax.broadcasted_iota(jnp.int32, (per, 8, 128), 1)
    low = s < 4
    first = s % 4 == 0
    last = s % 4 == 3
    f = pl.program_id(0)

    def halves(v):
        v = v.reshape(per, 2, 8, 128)
        return v[:, 0], v[:, 1]

    def window(a):
        return pl.ds(pl.multiple_of(a * span, span), span)

    def across(here, a, k):
        at = pl.ds(pl.multiple_of(a * 8, 8), 8)
        left = left_ref[k, at, :].astype(F32)[None]
        right = right_ref[k, at, :].astype(F32)[None]
        result = []
        for h, p in enumerate(here):
            near = jnp.where(first[:1], left if h == 0 else roll(left, 7), 0.0)
            far = jnp.where(last[:1], roll(right, 3 - h), 0.0)
            up = jnp.where(last, roll(p, 3), 0.0)
            down = jnp.where(first, roll(p, 5), 0.0)
            up = jnp.concatenate([up[1:], far], axis=0)
            down = jnp.concatenate([near, down[:-1]], axis=0)
            result.append(p + up + down)
        return result

    def rims(k, p0, p1):
        rim_ref[k, 0] = p0.reshape(per * 8, 128)
        rim_ref[k, 1] = p1.reshape(per * 8, 128)
        p0 = p0.reshape(per // 2, 2, 8, 128)
        p1 = p1.reshape(per // 2, 2, 8, 128)
        half = low[: per // 2]
        head_ref[k] = (
            jnp.where(half, p0[:, 0], roll(p0[:, 1], 4)).reshape(per * 4, 128).astype(BF16)
        )
        tail_ref[k] = (
            jnp.where(half, roll(p1[:, 0], 4), p1[:, 1]).reshape(per * 4, 128).astype(BF16)
        )

    def sweep(load, k, put):
        start, p1 = across(load(0), 0, k)

        def step(a, carry):
            y0, before = carry
            p0, p1 = across(load(a), a, k)
            put(a - 1, y0, before + jnp.where(low, 0.0, roll(p0, 4)))
            return p0 + jnp.where(low, roll(before, 4), 0.0), p1

        y0, p1 = lax.fori_loop(1, count, step, (start, p1))
        put(count - 1, y0, p1)
        rims(k, start, p1)

    def joined(y0, y1):
        return jnp.stack([y0, y1], axis=1).reshape(span, 128)

    @pl.when(f == 0)
    def _():
        def mass_at(a):
            m0, m1 = halves(m_ref[window(a), :])
            return m0 * q_ref[0][None], m1 * q_ref[1][None]

        def put(a, y0, y1):
            inv_ref[window(a), :] = section_step / joined(y0, y1)

        sweep(mass_at, fields, put)
        top = pl.ds(0, span)
        v0, v1 = halves(inv_ref[top, :])
        inv_ref[top, :] = joined(jnp.zeros_like(v0), v1)
        end = pl.ds(rows - span, span)
        v0, v1 = halves(inv_ref[end, :])
        inv_ref[end, :] = joined(v0, jnp.zeros_like(v1))

    def put(a, y0, y1):
        y = x_ref[0, window(a), :] + joined(y0, y1) * inv_ref[window(a), :]
        o_ref[0, window(a), :] = y.astype(o_ref.dtype)

    sweep(lambda a: halves(t_ref[0, window(a), :].astype(F32)), f, put)


def section_of(t, x, mass, left, right, rows_a):
    fields, rows, levels = x.shape
    per = rows // rows_a // 16
    whole = lambda a: pl.BlockSpec(a.shape, lambda f: (0,) * a.ndim)
    quad = jnp.asarray(row_tables()[12:14])
    one = pl.BlockSpec((1, rows, levels), lambda f: (f, 0, 0))
    edge = jax.ShapeDtypeStruct((fields + 1, per * 4, levels), BF16)
    rim = jax.ShapeDtypeStruct((fields + 1, 2, per * 8, levels), F32)
    section, rim, head, tail = pl.pallas_call(
        lambda *refs: section_body(*refs, per=per),
        grid=(fields,),
        in_specs=[one, one] + [whole(a) for a in (mass, quad, left, right)],
        out_specs=[
            one,
            whole(rim),
            whole(edge),
            whole(edge),
        ],
        out_shape=[
            jax.ShapeDtypeStruct(x.shape, BF16),
            rim,
            edge,
            edge,
        ],
        scratch_shapes=[pltpu.VMEM((rows, levels), F32)],
        name="section",
        compiler_params=pltpu.CompilerParams(vmem_limit_bytes=56 << 20),
    )(t, x, mass, quad, left, right)
    return section, rim, head, tail


def places_body(owner_ref, o_ref, *, devices, capacity):
    cols = owner_ref.shape[0]
    owner = owner_ref[...]
    hits = owner == lax.broadcasted_iota(jnp.int32, (cols, devices), 1)
    hits = jnp.where(hits, 1.0, 0.0)
    before = lax.broadcasted_iota(jnp.int32, (cols, cols), 0) > lax.broadcasted_iota(
        jnp.int32, (cols, cols), 1
    )
    before = jnp.where(before, 1.0, 0.0).astype(BF16)
    earlier = jnp.dot(before, hits.astype(BF16), preferred_element_type=F32)
    slot = jnp.sum(hits * earlier, axis=1, keepdims=True).astype(jnp.int32)
    o_ref[...] = owner * capacity + slot


def places(owner, devices, capacity):
    return pl.pallas_call(
        lambda a, o: places_body(a, o, devices=devices, capacity=capacity),
        out_shape=jax.ShapeDtypeStruct(owner.shape, jnp.int32),
        name="places",
        compiler_params=pltpu.CompilerParams(vmem_limit_bytes=60 << 20),
    )(owner)


def first_body(s_ref, w_ref, b_ref, o_ref, w2_ref):
    width = s_ref.shape[1]
    rest = w_ref.shape[0] - width
    y = jnp.dot(s_ref[...], w_ref[:width, :], preferred_element_type=F32) + b_ref[...]
    o_ref[...] = y.astype(BF16)
    w2_ref[:rest, :] = w_ref[width:, :]
    w2_ref[rest:, :] = jnp.zeros((w2_ref.shape[0] - rest, w2_ref.shape[1]), BF16)


def first_part(state, weight, bias, padded):
    cols, width = state.shape
    depth, hidden = weight.shape
    block = 512
    return pl.pallas_call(
        first_body,
        grid=(hidden // block,),
        in_specs=[
            pl.BlockSpec((cols, width), lambda i: (0, 0)),
            pl.BlockSpec((depth, block), lambda i: (0, i)),
            pl.BlockSpec((1, block), lambda i: (0, i)),
        ],
        out_specs=[
            pl.BlockSpec((cols, block), lambda i: (0, i)),
            pl.BlockSpec((padded, block), lambda i: (0, i)),
        ],
        out_shape=[
            jax.ShapeDtypeStruct((cols, hidden), BF16),
            jax.ShapeDtypeStruct((padded, hidden), BF16),
        ],
        name="first_part",
        compiler_params=pltpu.CompilerParams(vmem_limit_bytes=56 << 20),
    )(state, weight, bias)


def finish_body(
    place_hbm, home_hbm, w_hbm, part_hbm, wo_hbm, x_hbm, rim_hbm, bo_ref, spread_hbm, above_hbm, below_hbm, out_hbm,
    place_ref, home_ref, w_ref, part_ref, wo_ref, x_ref, rim_ref, spread_ref, above_ref, below_ref,
    sel_ref, aux_ref, o_ref, sem, out_sem, *, block
):
    fields, rows, levels = x_ref.shape
    cols = place_ref.shape[0]
    steps = cols // block
    half = home_ref.shape[1] // 2
    hidden_half = w_ref.shape[1] // 2

    copies = {}

    def fetch(name, src, dst):
        copies[name] = pltpu.make_async_copy(src, dst, sem.at[len(copies)])
        copies[name].start()

    def rows_of(k, scale=1):
        return pl.ds(k * block * scale, block * scale)

    def columns(k, width):
        return pl.ds(k * width, width)

    fetch("place", place_hbm, place_ref)
    for k in (0, 1):
        fetch(f"home{k}", home_hbm.at[:, columns(k, half)], home_ref.at[:, columns(k, half)])

    per = rim_ref.shape[2] // 8
    low = lax.broadcasted_iota(jnp.int32, (per // 2, 8, 128), 1) < 4

    def patch(h, halo, start):
        def total(k):
            p = halo[k].astype(F32).reshape(per // 2, 8, 128)
            q = roll(p, 4)
            if h == 0:
                add = jnp.stack([jnp.where(low, p, 0.0), jnp.where(low, q, 0.0)], axis=1)
            else:
                add = jnp.stack([jnp.where(low, 0.0, q), jnp.where(low, 0.0, p)], axis=1)
            return rim_ref[k, h].reshape(per, 8, 128) + add.reshape(per, 8, 128)

        scale = section_step / total(fields)
        to = pl.ds(start, per * 16)
        for f in range(fields):
            gain = total(f) * scale
            none = jnp.zeros_like(gain)
            both = jnp.stack([gain, none] if h == 0 else [none, gain], axis=1)
            o_ref[f, to, :] = o_ref[f, to, :] + both.reshape(per * 16, 128)

    copies["place"].wait()
    wide = lax.broadcasted_iota(jnp.int32, (block, sel_ref.shape[1]), 1)
    for k in range(steps):
        sel_ref[rows_of(k), :] = jnp.where(place_ref[rows_of(k), :] == wide, 1.0, 0.0).astype(BF16)
    for k in (0, 1):
        copies[f"home{k}"].wait()
        if k == 0:
            for n in (0, 1):
                fetch(f"w{n}", w_hbm.at[:, columns(n, hidden_half)], w_ref.at[:, columns(n, hidden_half)])
            fetch("part0", part_hbm.at[rows_of(0), :], part_ref.at[rows_of(0), :])
            fetch("wo", wo_hbm, wo_ref)
        else:
            fetch("spread", spread_hbm, spread_ref)
            fetch("x0", x_hbm.at[:, rows_of(0, 4), :], x_ref.at[:, rows_of(0, 4), :])
            fetch("rim", rim_hbm, rim_ref)
            fetch("above", above_hbm, above_ref)
            fetch("below", below_hbm, below_ref)
            for m in range(1, steps):
                fetch(f"part{m}", part_hbm.at[rows_of(m), :], part_ref.at[rows_of(m), :])
                fetch(f"x{m}", x_hbm.at[:, rows_of(m, 4), :], x_ref.at[:, rows_of(m, 4), :])
        aux_ref[:, k * half : (k + 1) * half] = jnp.dot(
            sel_ref[...], home_ref[:, k * half : (k + 1) * half], preferred_element_type=F32
        ).astype(BF16)
    group = spread_ref.shape[1]
    outs = []
    for k in range(steps):
        at = rows_of(k)
        copies[f"part{k}"].wait()
        if k == 0:
            for name in ("w0", "w1", "wo"):
                copies[name].wait()
        v = part_ref[at, :].astype(F32) + jnp.dot(aux_ref[at, :], w_ref[...], preferred_element_type=F32)
        v = 0.5 * v
        hidden = (v + v * jnp.tanh(v)).astype(BF16)
        inc = jnp.dot(hidden, wo_ref[...], preferred_element_type=F32) + bo_ref[...]
        inc = inc.astype(BF16)
        copies[f"x{k}"].wait()
        if k == 0:
            for name in ("spread", "rim", "above", "below"):
                copies[name].wait()
        for g in range(block // group):
            wide = jnp.dot(
                spread_ref[...], inc[g * group : (g + 1) * group], preferred_element_type=F32
            )
            to = pl.ds((k * block + g * group) * 4, group * 4)
            for f in range(fields):
                o_ref[f, to, :] = x_ref[f, to, :].astype(F32) + wide[:, f * levels : (f + 1) * levels]
        if k == 0:
            patch(0, above_ref, 0)
        if k == steps - 1:
            patch(1, below_ref, rows - per * 16)
        done = pltpu.make_async_copy(
            o_ref.at[:, rows_of(k, 4), :], out_hbm.at[:, rows_of(k, 4), :], out_sem.at[k]
        )
        done.start()
        outs.append(done)
    for done in outs:
        done.wait()


def spread_table(group):
    spread = np.zeros((group * 4, group), np.float32)
    for r in range(group * 4):
        e, i, j = r // 16, (r // 4) % 4, r % 4
        spread[r, e * 4 + (i // 2) * 2 + j // 2] = 1.0
    return spread


def finish(place, home, weight, part, weight_out, bias_out, x, rim, above, below):
    cols, slots = place.shape[0], home.shape[0]
    fields, rows, levels = x.shape
    block = 256
    steps = cols // block
    spread = jnp.asarray(spread_table(128), BF16)
    far = pl.BlockSpec(memory_space=pltpu.HBM)
    first = (place, home, weight, part, weight_out, x, rim)
    after = (spread, above, below)
    return pl.pallas_call(
        lambda *refs: finish_body(*refs, block=block),
        in_specs=[far] * len(first) + [pl.BlockSpec(bias_out.shape, lambda: (0, 0))] + [far] * len(after),
        out_specs=far,
        out_shape=jax.ShapeDtypeStruct(x.shape, F32),
        scratch_shapes=[pltpu.VMEM(a.shape, a.dtype) for a in (*first, *after)]
        + [
            pltpu.VMEM((cols, slots), BF16),
            pltpu.VMEM((cols, home.shape[1]), BF16),
            pltpu.VMEM(x.shape, F32),
            pltpu.SemaphoreType.DMA((10 + 2 * steps,)),
            pltpu.SemaphoreType.DMA((steps,)),
        ],
        name="finish",
        compiler_params=pltpu.CompilerParams(vmem_limit_bytes=52 << 20),
    )(*first, bias_out, *after)


def shards(
    prognostic, layer_mass, column_aux, group_owner, weight_in, bias_in, weight_out, bias_out
):
    fields, rows_a, rows_b, _, _, levels = prognostic.shape
    n_curve, n_sub = lax.axis_size("curve"), lax.axis_size("sub")
    devices = n_curve * n_sub
    capacity = column_aux.shape[0] // devices
    aux_width = column_aux.shape[1]
    padded = -(-aux_width // 128) * 128
    rows = rows_a * rows_b * 16

    home = turn(column_aux.T, padded).reshape(devices, capacity, padded)
    home = lax.all_to_all(home, AXES, split_axis=0, concat_axis=0, tiled=True)
    home = home.reshape(devices * capacity, padded)

    x = prognostic.reshape(fields, rows, levels)
    mass = layer_mass.reshape(rows, levels)
    tend, state, left_out, right_out = tendencies(x, mass, rows_a)

    def ahead(n):
        return [(i, (i + 1) % n) for i in range(n)]

    def back(n):
        return [((i + 1) % n, i) for i in range(n)]

    left = lax.ppermute(right_out, "sub", ahead(n_sub))
    right = lax.ppermute(left_out, "sub", back(n_sub))
    section, rim, head, tail = section_of(tend, x, mass, left, right, rows_a)
    above = lax.ppermute(tail, "curve", ahead(n_curve))
    below = lax.ppermute(head, "curve", back(n_curve))

    place = places(group_owner, devices, capacity)
    part, weight_aux = first_part(state, weight_in, bias_in[None], padded)
    out = finish(place, home, weight_aux, part, weight_out, bias_out[None], section, rim, above, below)
    return out.reshape(prognostic.shape)


def solution(mesh):
    return jax.shard_map(
        shards,
        mesh=mesh,
        in_specs=(
            P(None, "curve", "sub", None, None, None),
            P("curve", "sub", None, None, None),
            P(("curve", "sub"), None),
            P(("curve", "sub"), None),
            P(),
            P(),
            P(),
            P(),
        ),
        out_specs=P(None, "curve", "sub", None, None, None),
        check_vma=False,
    )
```

```python
import jax
import jax.numpy as jnp
import numpy as np
from jax import lax
from jax.experimental import pallas as pl
from jax.experimental.pallas import tpu as pltpu
from jax.sharding import PartitionSpec as P

section_step = 0.1
AXES = ("curve", "sub")
F32 = jnp.float32
BF16 = jnp.bfloat16


def node_tables():
    nodes = np.array([-1.0, -1.0 / np.sqrt(5.0), 1.0 / np.sqrt(5.0), 1.0])
    quadrature = np.array([1.0 / 6.0, 5.0 / 6.0, 5.0 / 6.0, 1.0 / 6.0])
    products = np.array(
        [np.prod([nodes[i] - nodes[k] for k in range(4) if k != i]) for i in range(4)]
    )
    derivative = np.zeros((4, 4))
    for i in range(4):
        for k in range(4):
            if i != k:
                derivative[i, k] = products[i] / (products[k] * (nodes[i] - nodes[k]))
            else:
                derivative[i, i] = sum(1.0 / (nodes[i] - nodes[m]) for m in range(4) if m != i)
    return derivative.astype(np.float32), quadrature.astype(np.float32)


def row_tables():
    d, w = node_tables()
    s = np.arange(8)
    i, j = s // 4, s % 4
    tables = []
    for half in (0, 2):
        for column in (i, 1 - i, 2 + i, 3 - i):
            tables.append(-d[half + i, column])
    for shift in range(4):
        tables.append(-d[j, (j - shift) % 4])
    for half in (0, 2):
        tables.append(w[half + i] * w[j])
    return np.repeat(np.stack(tables)[:, :, None], 128, axis=2).astype(np.float32)


def lane_rows(x):
    return lax.broadcasted_iota(jnp.int32, x, len(x) - 2)


def roll(x, shift):
    return pltpu.roll(x, shift % 8, axis=1)


def turn_body(x_ref, o_ref):
    width = x_ref.shape[0]
    o_ref[:, :width] = x_ref[...].T
    o_ref[:, width:] = jnp.zeros((o_ref.shape[0], o_ref.shape[1] - width), BF16)


def turn(aux_t, padded):
    width, rows = aux_t.shape
    block = rows // 2
    return pl.pallas_call(
        turn_body,
        grid=(rows // block,),
        in_specs=[pl.BlockSpec((width, block), lambda i: (0, i))],
        out_specs=pl.BlockSpec((block, padded), lambda i: (i, 0)),
        out_shape=jax.ShapeDtypeStruct((rows, padded), BF16),
        name="turn",
        compiler_params=pltpu.CompilerParams(vmem_limit_bytes=56 << 20),
    )(aux_t)


def tend_body(x_ref, m_ref, q_ref, deriv_ref, pick_ref, o_ref, c_ref, l_ref, r_ref):
    fields, rows, levels = x_ref.shape
    group = q_ref.shape[0]
    cells = group // 4
    lines = (pick_ref.shape[0] - cells) // 2

    for g in range(rows // group):
        at = pl.ds(g * group, group)
        cell_at = pl.ds(g * cells, cells)
        line_at = pl.ds(g * lines, lines)

        def picked(first, second):
            y = jnp.dot(
                pick_ref[...], jnp.concatenate([first, second], axis=1), preferred_element_type=F32
            )
            return y[:cells, :levels], y[cells:, levels:].astype(BF16)

        w = m_ref[at, :] * q_ref[...]
        wb = w.astype(BF16)
        mass, edge = picked(wb, wb)
        inv = 1.0 / mass
        l_ref[fields, line_at, :] = edge[:lines]
        r_ref[fields, line_at, :] = edge[lines:]
        uw = x_ref[0, at, :] * w
        vw = x_ref[1, at, :] * w
        for pair in range(0, fields, 2):
            both = (x_ref[pair, at, :], x_ref[pair + 1, at, :])
            high = jnp.concatenate([x.astype(BF16) for x in both], axis=1)
            low = jnp.concatenate([(x - x.astype(BF16).astype(F32)).astype(BF16) for x in both], axis=1)
            d = jnp.dot(
                deriv_ref[...], jnp.concatenate([high, high, low], axis=0), preferred_element_type=F32
            )
            for k, x in enumerate(both):
                f = pair + k
                lanes = slice(k * levels, (k + 1) * levels)
                out = (uw * d[:group, lanes] + vw * d[group:, lanes]).astype(BF16)
                xw = (uw if f == 0 else vw if f == 1 else x * w).astype(BF16)
                o_ref[f, at, :] = out
                mean, edge = picked(xw, out)
                c_ref[cell_at, f * levels : (f + 1) * levels] = (mean * inv).astype(BF16)
                l_ref[f, line_at, :] = edge[:lines]
                r_ref[f, line_at, :] = edge[lines:]


def derivative_table(group):
    d = node_tables()[0]
    r = np.arange(group)
    same = (r[:, None] // 16) == (r[None, :] // 16)
    i, j = (r // 4) % 4, r % 4
    along_first = np.where(same & (j[:, None] == j[None, :]), d[i[:, None], i[None, :]], 0.0)
    along_second = np.where(same & (i[:, None] == i[None, :]), d[j[:, None], j[None, :]], 0.0)
    return -np.concatenate([along_first, along_second], axis=0)


def pick_table(group, span):
    r = np.arange(group)
    cells = np.zeros((group // 4, group), np.float32)
    cells[(r // 16) * 4 + ((r // 8) % 2) * 2 + (r % 4) // 2, r] = 1.0
    lines = [np.zeros((group // span * 8, group), np.float32) for _ in range(2)]
    for a in range(group // span):
        for i in range(4):
            to = a * 8 + (i % 2) * 4 + i // 2
            lines[0][to, a * span + i * 4] = 1.0
            lines[1][to, (a + 1) * span - 16 + i * 4 + 3] = 1.0
    return np.concatenate([cells] + lines, axis=0)


def tendencies(x, mass, rows_a):
    fields, rows, levels = x.shape
    span = rows // rows_a
    group = 2 * span
    lot = 4
    block = lot * span
    quad = np.tile(row_tables()[12:14].reshape(16, 128), (group // 16, 1))
    deriv = derivative_table(group)
    top = deriv.astype(jnp.bfloat16)
    deriv = jnp.asarray(np.concatenate([top, (deriv - top.astype(np.float64)).astype(jnp.bfloat16), top], axis=1))
    pick = jnp.asarray(pick_table(group, span), BF16)
    edge = jax.ShapeDtypeStruct((fields + 1, rows_a * 8, levels), BF16)
    whole = lambda a: pl.BlockSpec(a.shape, lambda i: (0, 0))
    return pl.pallas_call(
        tend_body,
        grid=(rows // block,),
        in_specs=[
            pl.BlockSpec((fields, block, levels), lambda i: (0, i, 0)),
            pl.BlockSpec((block, levels), lambda i: (i, 0)),
            whole(quad),
            whole(deriv),
            whole(pick),
        ],
        out_specs=[
            pl.BlockSpec((fields, block, levels), lambda i: (0, i, 0)),
            pl.BlockSpec((block // 4, fields * levels), lambda i: (i, 0)),
            pl.BlockSpec((fields + 1, lot * 8, levels), lambda i: (0, i, 0)),
            pl.BlockSpec((fields + 1, lot * 8, levels), lambda i: (0, i, 0)),
        ],
        out_shape=[
            jax.ShapeDtypeStruct((fields, rows, levels), BF16),
            jax.ShapeDtypeStruct((rows // 4, fields * levels), BF16),
            edge,
            edge,
        ],
        name="tendencies",
        compiler_params=pltpu.CompilerParams(vmem_limit_bytes=56 << 20),
    )(x, mass, jnp.asarray(quad), deriv, pick)


def section_body(
    t_ref, x_ref, m_ref, q_ref, left_ref, right_ref, o_ref, head_ref, tail_ref, inv_ref, rim_ref, *, per
):
    rows = x_ref.shape[1]
    span = per * 16
    count = rows // span
    fields = head_ref.shape[0] - 1
    s = lax.broadcasted_iota(jnp.int32, (per, 8, 128), 1)
    low = s < 4
    first = s % 4 == 0
    last = s % 4 == 3
    f = pl.program_id(0)

    def halves(v):
        v = v.reshape(per, 2, 8, 128)
        return v[:, 0], v[:, 1]

    def window(a):
        return pl.ds(pl.multiple_of(a * span, span), span)

    def across(here, a, k):
        at = pl.ds(pl.multiple_of(a * 8, 8), 8)
        left = left_ref[k, at, :].astype(F32)[None]
        right = right_ref[k, at, :].astype(F32)[None]
        result = []
        for h, p in enumerate(here):
            near = jnp.where(first[:1], left if h == 0 else roll(left, 7), 0.0)
            far = jnp.where(last[:1], roll(right, 3 - h), 0.0)
            up = jnp.where(last, roll(p, 3), 0.0)
            down = jnp.where(first, roll(p, 5), 0.0)
            up = jnp.concatenate([up[1:], far], axis=0)
            down = jnp.concatenate([near, down[:-1]], axis=0)
            result.append(p + up + down)
        return result

    def rims(k, p0, p1):
        both = jnp.concatenate([p0.reshape(per * 8, 128), p1.reshape(per * 8, 128)], axis=0).astype(BF16)
        if isinstance(k, int):
            rim_ref[...] = both
        else:
            o_ref[0, rows : rows + per * 16, :] = both
            o_ref[0, rows + per * 16 :, :] = rim_ref[...]
        p0 = p0.reshape(per // 2, 2, 8, 128)
        p1 = p1.reshape(per // 2, 2, 8, 128)
        half = low[: per // 2]
        head_ref[k] = (
            jnp.where(half, p0[:, 0], roll(p0[:, 1], 4)).reshape(per * 4, 128).astype(BF16)
        )
        tail_ref[k] = (
            jnp.where(half, roll(p1[:, 0], 4), p1[:, 1]).reshape(per * 4, 128).astype(BF16)
        )

    def sweep(load, k, put):
        start, p1 = across(load(0), 0, k)

        def step(a, carry):
            y0, before = carry
            p0, p1 = across(load(a), a, k)
            put(a - 1, y0, before + jnp.where(low, 0.0, roll(p0, 4)))
            return p0 + jnp.where(low, roll(before, 4), 0.0), p1

        y0, p1 = lax.fori_loop(1, count, step, (start, p1))
        put(count - 1, y0, p1)
        rims(k, start, p1)

    def joined(y0, y1):
        return jnp.stack([y0, y1], axis=1).reshape(span, 128)

    @pl.when(f == 0)
    def _():
        def mass_at(a):
            m0, m1 = halves(m_ref[window(a), :])
            return m0 * q_ref[0][None], m1 * q_ref[1][None]

        def put(a, y0, y1):
            inv_ref[window(a), :] = section_step / joined(y0, y1)

        sweep(mass_at, fields, put)
        top = pl.ds(0, span)
        v0, v1 = halves(inv_ref[top, :])
        inv_ref[top, :] = joined(jnp.zeros_like(v0), v1)
        end = pl.ds(rows - span, span)
        v0, v1 = halves(inv_ref[end, :])
        inv_ref[end, :] = joined(v0, jnp.zeros_like(v1))

    def put(a, y0, y1):
        y = x_ref[0, window(a), :] + joined(y0, y1) * inv_ref[window(a), :]
        o_ref[0, window(a), :] = y.astype(o_ref.dtype)

    sweep(lambda a: halves(t_ref[0, window(a), :].astype(F32)), f, put)


def section_of(t, x, mass, left, right, rows_a):
    fields, rows, levels = x.shape
    per = rows // rows_a // 16
    whole = lambda a: pl.BlockSpec(a.shape, lambda f: (0,) * a.ndim)
    quad = jnp.asarray(row_tables()[12:14])
    one = pl.BlockSpec((1, rows, levels), lambda f: (f, 0, 0))
    edge = jax.ShapeDtypeStruct((fields + 1, per * 4, levels), BF16)
    tall = rows + per * 32
    return pl.pallas_call(
        lambda *refs: section_body(*refs, per=per),
        grid=(fields,),
        in_specs=[one, one] + [whole(a) for a in (mass, quad, left, right)],
        out_specs=[
            pl.BlockSpec((1, tall, levels), lambda f: (f, 0, 0)),
            whole(edge),
            whole(edge),
        ],
        out_shape=[
            jax.ShapeDtypeStruct((fields, tall, levels), BF16),
            edge,
            edge,
        ],
        scratch_shapes=[pltpu.VMEM((rows, levels), F32), pltpu.VMEM((per * 16, levels), BF16)],
        name="section",
        compiler_params=pltpu.CompilerParams(vmem_limit_bytes=56 << 20),
    )(t, x, mass, quad, left, right)


def places_body(owner_ref, o_ref, *, devices, capacity):
    cols = owner_ref.shape[0]
    owner = owner_ref[...]
    hits = owner == lax.broadcasted_iota(jnp.int32, (cols, devices), 1)
    hits = jnp.where(hits, 1.0, 0.0)
    before = lax.broadcasted_iota(jnp.int32, (cols, cols), 0) > lax.broadcasted_iota(
        jnp.int32, (cols, cols), 1
    )
    before = jnp.where(before, 1.0, 0.0).astype(BF16)
    earlier = jnp.dot(before, hits.astype(BF16), preferred_element_type=F32)
    slot = jnp.sum(hits * earlier, axis=1, keepdims=True).astype(jnp.int32)
    o_ref[...] = owner * capacity + slot


def places(owner, devices, capacity):
    return pl.pallas_call(
        lambda a, o: places_body(a, o, devices=devices, capacity=capacity),
        out_shape=jax.ShapeDtypeStruct(owner.shape, jnp.int32),
        name="places",
        compiler_params=pltpu.CompilerParams(vmem_limit_bytes=60 << 20),
    )(owner)


def first_body(s_ref, w_ref, b_ref, wo_ref, o_ref, w2_ref, *, padded):
    width = s_ref.shape[1]
    rest = w_ref.shape[0] - width
    y = jnp.dot(s_ref[...], w_ref[:width, :], preferred_element_type=F32) + b_ref[...]
    o_ref[...] = y.astype(BF16)
    w2_ref[:rest, :] = w_ref[width:, :]
    w2_ref[rest:padded, :] = jnp.zeros((padded - rest, w2_ref.shape[1]), BF16)
    w2_ref[padded:, :] = wo_ref[...]


def first_part(state, weight, bias, weight_out, padded):
    cols, width = state.shape
    depth, hidden = weight.shape
    block = weight_out.shape[1]
    tall = padded + block
    return pl.pallas_call(
        lambda *refs: first_body(*refs, padded=padded),
        grid=(hidden // block,),
        in_specs=[
            pl.BlockSpec((cols, width), lambda i: (0, 0)),
            pl.BlockSpec((depth, block), lambda i: (0, i)),
            pl.BlockSpec((1, block), lambda i: (0, i)),
            pl.BlockSpec((block, block), lambda i: (i, 0)),
        ],
        out_specs=[
            pl.BlockSpec((cols, block), lambda i: (0, i)),
            pl.BlockSpec((tall, block), lambda i: (0, i)),
        ],
        out_shape=[
            jax.ShapeDtypeStruct((cols, hidden), BF16),
            jax.ShapeDtypeStruct((tall, hidden), BF16),
        ],
        name="first_part",
        compiler_params=pltpu.CompilerParams(vmem_limit_bytes=56 << 20),
    )(state, weight, bias, weight_out)


def finish_body(
    home_ref, place_ref, w_hbm, part_hbm, bo_ref, x_hbm, above_ref, below_ref, out_hbm,
    w_ref, part_ref, x_ref, sel_ref, aux_ref, spread_ref, o_ref, sem, out_sem, *, block
):
    fields, rows, levels = o_ref.shape
    cols = place_ref.shape[0]
    per = above_ref.shape[1] // 4
    edge_rows = pl.ds(rows, per * 32)
    steps = cols // block
    half = home_ref.shape[1] // 2
    hidden_half = w_ref.shape[1] // 2

    def rows_of(k, scale=1):
        return pl.ds(k * block * scale, block * scale)

    def columns(k, width):
        return pl.ds(k * width, width)

    def jobs():
        for k in (0, 1):
            yield f"w{k}", w_hbm.at[:, columns(k, hidden_half)], w_ref.at[:, columns(k, hidden_half)]
        yield "edge", x_hbm.at[:, edge_rows, :], x_ref.at[:, edge_rows, :]
        for k in range(steps):
            yield f"part{k}", part_hbm.at[rows_of(k), :], part_ref.at[rows_of(k), :]
            yield f"x{k}", x_hbm.at[:, rows_of(k, 4), :], x_ref.at[:, rows_of(k, 4), :]

    def each(names, act):
        for n, (name, src, dst) in enumerate(jobs()):
            if name in names:
                act(pltpu.make_async_copy(src, dst, sem.at[n]))

    def fetch(*names):
        each(names, lambda copy: copy.start())

    def wait(*names):
        each(names, lambda copy: copy.wait())

    later = [f"{kind}{k}" for k in range(1, steps) for kind in ("part", "x")]
    fetch("w0", "w1", "part0", "edge", "x0", *later)

    low = lax.broadcasted_iota(jnp.int32, (per // 2, 8, 128), 1) < 4

    def patch(h, halo, start):
        def total(k):
            p = halo[k].astype(F32).reshape(per // 2, 8, 128)
            q = roll(p, 4)
            if h == 0:
                add = jnp.stack([jnp.where(low, p, 0.0), jnp.where(low, q, 0.0)], axis=1)
            else:
                add = jnp.stack([jnp.where(low, 0.0, q), jnp.where(low, 0.0, p)], axis=1)
            own = pl.ds(rows + (per * 16 if k == fields else 0) + h * per * 8, per * 8)
            own = x_ref[0 if k == fields else k, own, :].astype(F32)
            return own.reshape(per, 8, 128) + add.reshape(per, 8, 128)

        scale = section_step / total(fields)
        to = pl.ds(start, per * 16)
        for f in range(fields):
            gain = total(f) * scale
            none = jnp.zeros_like(gain)
            both = jnp.stack([gain, none] if h == 0 else [none, gain], axis=1)
            o_ref[f, to, :] = o_ref[f, to, :] + both.reshape(per * 16, 128)

    wide = lax.broadcasted_iota(jnp.int32, (block, sel_ref.shape[1]), 1)
    for k in range(steps):
        sel_ref[rows_of(k), :] = jnp.where(place_ref[rows_of(k), :] == wide, 1.0, 0.0).astype(BF16)
    def gather(k, carry):
        lanes = pl.ds(pl.multiple_of(k * half, 128), half)
        aux_ref[:, lanes] = jnp.dot(
            sel_ref[...], home_ref[:, lanes], preferred_element_type=F32
        ).astype(BF16)
        return carry

    lax.fori_loop(0, 2, gather, 0)
    group = 128
    row = lax.broadcasted_iota(jnp.int32, (group * 4, group), 0)
    cell = (row // 16) * 4 + ((row // 8) % 2) * 2 + (row % 4) // 2
    spread = jnp.where(cell == lax.broadcasted_iota(jnp.int32, cell.shape, 1), 1.0, 0.0).astype(BF16)
    spread_ref[...] = spread
    padded = home_ref.shape[1]
    width = bo_ref.shape[1]
    wait("w0", "w1", "part0", "edge")

    def out_copy(k):
        at = pl.ds(pl.multiple_of(k * block * 4, block * 4), block * 4)
        return pltpu.make_async_copy(o_ref.at[:, at, :], out_hbm.at[:, at, :], out_sem.at[k])

    def layers(k, carry):
        at = pl.ds(pl.multiple_of(k * block, block), block)

        @pl.when(k == 1)
        def _():
            wait(*[f"part{m}" for m in range(1, steps)])

        v = part_ref[at, :].astype(F32) + jnp.dot(
            aux_ref[at, :], w_ref[:padded, :], preferred_element_type=F32
        )
        v = 0.5 * v
        hidden = (v + v * jnp.tanh(v)).astype(BF16)
        inc = bo_ref[...]
        for n in range(hidden.shape[1] // width):
            lanes = slice(n * width, (n + 1) * width)
            inc = inc + jnp.dot(hidden[:, lanes], w_ref[padded:, lanes], preferred_element_type=F32)
        inc = inc.astype(BF16)

        @pl.when(k == 0)
        def _():
            wait(*[f"x{m}" for m in range(steps)])

        for g in range(block // group):
            wide = jnp.dot(
                spread_ref[...], inc[g * group : (g + 1) * group], preferred_element_type=F32
            )
            to = pl.ds(pl.multiple_of((k * block + g * group) * 4, group * 4), group * 4)
            for f in range(fields):
                o_ref[f, to, :] = x_ref[f, to, :].astype(F32) + wide[:, f * levels : (f + 1) * levels]

        @pl.when(k == 0)
        def _():
            patch(0, above_ref, 0)

        @pl.when(k == steps - 1)
        def _():
            patch(1, below_ref, rows - per * 16)

        out_copy(k).start()
        return carry

    lax.fori_loop(0, steps, layers, 0)
    for k in range(steps):
        out_copy(k).wait()


def finish(home, place, weights, part, bias_out, x, above, below):
    cols, slots = place.shape[0], home.shape[0]
    fields, levels = x.shape[0], x.shape[2]
    result = (fields, cols * 4, levels)
    block = 384
    steps = cols // block
    far = pl.BlockSpec(memory_space=pl.ANY)
    near = pl.BlockSpec(memory_space=pltpu.VMEM)
    return pl.pallas_call(
        lambda *refs: finish_body(*refs, block=block),
        in_specs=[near, near, far, far, near, far, near, near],
        out_specs=far,
        out_shape=jax.ShapeDtypeStruct(result, F32),
        scratch_shapes=[pltpu.VMEM(a.shape, a.dtype) for a in (weights, part, x)]
        + [
            pltpu.VMEM((cols, slots), BF16),
            pltpu.VMEM((cols, home.shape[1]), BF16),
            pltpu.VMEM((512, 128), BF16),
            pltpu.VMEM(result, F32),
            pltpu.SemaphoreType.DMA((3 + 2 * steps,)),
            pltpu.SemaphoreType.DMA((steps,)),
        ],
        name="finish",
        compiler_params=pltpu.CompilerParams(vmem_limit_bytes=48 << 20),
    )(home, place, weights, part, bias_out, x, above, below)


def shards(
    prognostic, layer_mass, column_aux, group_owner, weight_in, bias_in, weight_out, bias_out
):
    fields, rows_a, rows_b, _, _, levels = prognostic.shape
    n_curve, n_sub = lax.axis_size("curve"), lax.axis_size("sub")
    devices = n_curve * n_sub
    capacity = column_aux.shape[0] // devices
    aux_width = column_aux.shape[1]
    padded = -(-aux_width // 128) * 128
    rows = rows_a * rows_b * 16

    home = turn(column_aux.T, padded).reshape(devices, capacity, padded)
    home = lax.all_to_all(home, AXES, split_axis=0, concat_axis=0, tiled=True)
    home = home.reshape(devices * capacity, padded)

    x = prognostic.reshape(fields, rows, levels)
    mass = layer_mass.reshape(rows, levels)
    tend, state, left_out, right_out = tendencies(x, mass, rows_a)

    def ahead(n):
        return [(i, (i + 1) % n) for i in range(n)]

    def back(n):
        return [((i + 1) % n, i) for i in range(n)]

    left = lax.ppermute(right_out, "sub", ahead(n_sub))
    right = lax.ppermute(left_out, "sub", back(n_sub))
    section, head, tail = section_of(tend, x, mass, left, right, rows_a)
    above = lax.ppermute(tail, "curve", ahead(n_curve))
    below = lax.ppermute(head, "curve", back(n_curve))

    place = places(group_owner, devices, capacity)
    part, weights = first_part(state, weight_in, bias_in[None], weight_out, padded)
    out = finish(home, place, weights, part, bias_out[None], section, above, below)
    return out.reshape(prognostic.shape)


def solution(mesh):
    return jax.shard_map(
        shards,
        mesh=mesh,
        in_specs=(
            P(None, "curve", "sub", None, None, None),
            P("curve", "sub", None, None, None),
            P(("curve", "sub"), None),
            P(("curve", "sub"), None),
            P(),
            P(),
            P(),
            P(),
        ),
        out_specs=P(None, "curve", "sub", None, None, None),
        check_vma=False,
    )
```

```python
import jax
import jax.numpy as jnp
import numpy as np
from jax import lax
from jax.experimental import pallas as pl
from jax.experimental.pallas import tpu as pltpu
from jax.sharding import PartitionSpec as P

section_step = 0.1
AXES = ("curve", "sub")
F32 = jnp.float32
BF16 = jnp.bfloat16


def node_tables():
    nodes = np.array([-1.0, -1.0 / np.sqrt(5.0), 1.0 / np.sqrt(5.0), 1.0])
    quadrature = np.array([1.0 / 6.0, 5.0 / 6.0, 5.0 / 6.0, 1.0 / 6.0])
    products = np.array(
        [np.prod([nodes[i] - nodes[k] for k in range(4) if k != i]) for i in range(4)]
    )
    derivative = np.zeros((4, 4))
    for i in range(4):
        for k in range(4):
            if i != k:
                derivative[i, k] = products[i] / (products[k] * (nodes[i] - nodes[k]))
            else:
                derivative[i, i] = sum(1.0 / (nodes[i] - nodes[m]) for m in range(4) if m != i)
    return derivative.astype(np.float32), quadrature.astype(np.float32)


def row_tables():
    d, w = node_tables()
    s = np.arange(8)
    i, j = s // 4, s % 4
    tables = []
    for half in (0, 2):
        for column in (i, 1 - i, 2 + i, 3 - i):
            tables.append(-d[half + i, column])
    for shift in range(4):
        tables.append(-d[j, (j - shift) % 4])
    for half in (0, 2):
        tables.append(w[half + i] * w[j])
    return np.repeat(np.stack(tables)[:, :, None], 128, axis=2).astype(np.float32)


def lane_rows(x):
    return lax.broadcasted_iota(jnp.int32, x, len(x) - 2)


def roll(x, shift):
    return pltpu.roll(x, shift % 8, axis=1)


def turn_body(x_hbm, o_hbm, x_ref, o_ref, in_sem, out_sem):
    pieces = in_sem.shape[0]
    width, rows = x_ref.shape
    n = rows // pieces

    def take(k):
        lanes = pl.ds(k * n, n)
        return pltpu.make_async_copy(x_hbm.at[:, lanes], x_ref.at[:, lanes], in_sem.at[k])

    def give(k):
        at = pl.ds(k * n, n)
        return pltpu.make_async_copy(o_ref.at[at, :], o_hbm.at[at, :], out_sem.at[k])

    for k in range(pieces):
        take(k).start()
    o_ref[:, width:] = jnp.zeros((rows, o_ref.shape[1] - width), BF16)
    for k in range(pieces):
        take(k).wait()
        at = slice(k * n, (k + 1) * n)
        o_ref[at, :width] = x_ref[:, at].T
        give(k).start()
    for k in range(pieces):
        give(k).wait()


def turn(aux_t, padded):
    width, rows = aux_t.shape
    pieces = 3
    far = pl.BlockSpec(memory_space=pltpu.HBM)
    return pl.pallas_call(
        turn_body,
        in_specs=[far],
        out_specs=far,
        out_shape=jax.ShapeDtypeStruct((rows, padded), BF16),
        scratch_shapes=[
            pltpu.VMEM((width, rows), BF16),
            pltpu.VMEM((rows, padded), BF16),
            pltpu.SemaphoreType.DMA((pieces,)),
            pltpu.SemaphoreType.DMA((pieces,)),
        ],
        name="turn",
        compiler_params=pltpu.CompilerParams(vmem_limit_bytes=56 << 20),
    )(aux_t)


def tend_body(x_ref, m_ref, q_ref, deriv_ref, pick_ref, o_ref, c_ref, l_ref, r_ref):
    fields, rows, levels = x_ref.shape
    group = q_ref.shape[0]
    cells = group // 4
    lines = (pick_ref.shape[0] - cells) // 2

    for g in range(rows // group):
        at = pl.ds(g * group, group)
        cell_at = pl.ds(g * cells, cells)
        line_at = pl.ds(g * lines, lines)

        def picked(first, second):
            y = jnp.dot(
                pick_ref[...], jnp.concatenate([first, second], axis=1), preferred_element_type=F32
            )
            return y[:cells, :levels], y[cells:, levels:].astype(BF16)

        w = m_ref[at, :] * q_ref[...]
        wb = w.astype(BF16)
        mass, edge = picked(wb, wb)
        inv = 1.0 / mass
        l_ref[fields, line_at, :] = edge[:lines]
        r_ref[fields, line_at, :] = edge[lines:]
        uw = x_ref[0, at, :] * w
        vw = x_ref[1, at, :] * w
        for pair in range(0, fields, 2):
            both = (x_ref[pair, at, :], x_ref[pair + 1, at, :])
            high = jnp.concatenate([x.astype(BF16) for x in both], axis=1)
            low = jnp.concatenate([(x - x.astype(BF16).astype(F32)).astype(BF16) for x in both], axis=1)
            d = jnp.dot(
                deriv_ref[...], jnp.concatenate([high, high, low], axis=0), preferred_element_type=F32
            )
            for k, x in enumerate(both):
                f = pair + k
                lanes = slice(k * levels, (k + 1) * levels)
                out = (uw * d[:group, lanes] + vw * d[group:, lanes]).astype(BF16)
                xw = (uw if f == 0 else vw if f == 1 else x * w).astype(BF16)
                o_ref[f, at, :] = out
                mean, edge = picked(xw, out)
                c_ref[cell_at, f * levels : (f + 1) * levels] = (mean * inv).astype(BF16)
                l_ref[f, line_at, :] = edge[:lines]
                r_ref[f, line_at, :] = edge[lines:]


def derivative_table(group):
    d = node_tables()[0]
    r = np.arange(group)
    same = (r[:, None] // 16) == (r[None, :] // 16)
    i, j = (r // 4) % 4, r % 4
    along_first = np.where(same & (j[:, None] == j[None, :]), d[i[:, None], i[None, :]], 0.0)
    along_second = np.where(same & (i[:, None] == i[None, :]), d[j[:, None], j[None, :]], 0.0)
    return -np.concatenate([along_first, along_second], axis=0)


def pick_table(group, span):
    r = np.arange(group)
    cells = np.zeros((group // 4, group), np.float32)
    cells[(r // 16) * 4 + ((r // 8) % 2) * 2 + (r % 4) // 2, r] = 1.0
    lines = [np.zeros((group // span * 8, group), np.float32) for _ in range(2)]
    for a in range(group // span):
        for i in range(4):
            to = a * 8 + (i % 2) * 4 + i // 2
            lines[0][to, a * span + i * 4] = 1.0
            lines[1][to, (a + 1) * span - 16 + i * 4 + 3] = 1.0
    return np.concatenate([cells] + lines, axis=0)


def tendencies(x, mass, rows_a):
    fields, rows, levels = x.shape
    span = rows // rows_a
    group = 2 * span
    lot = 4
    block = lot * span
    quad = np.tile(row_tables()[12:14].reshape(16, 128), (group // 16, 1))
    deriv = derivative_table(group)
    top = deriv.astype(jnp.bfloat16)
    deriv = jnp.asarray(np.concatenate([top, (deriv - top.astype(np.float64)).astype(jnp.bfloat16), top], axis=1))
    pick = jnp.asarray(pick_table(group, span), BF16)
    edge = jax.ShapeDtypeStruct((fields + 1, rows_a * 8, levels), BF16)
    whole = lambda a: pl.BlockSpec(a.shape, lambda i: (0, 0))
    return pl.pallas_call(
        tend_body,
        grid=(rows // block,),
        in_specs=[
            pl.BlockSpec((fields, block, levels), lambda i: (0, i, 0)),
            pl.BlockSpec((block, levels), lambda i: (i, 0)),
            whole(quad),
            whole(deriv),
            whole(pick),
        ],
        out_specs=[
            pl.BlockSpec((fields, block, levels), lambda i: (0, i, 0)),
            pl.BlockSpec((block // 4, fields * levels), lambda i: (i, 0)),
            pl.BlockSpec((fields + 1, lot * 8, levels), lambda i: (0, i, 0)),
            pl.BlockSpec((fields + 1, lot * 8, levels), lambda i: (0, i, 0)),
        ],
        out_shape=[
            jax.ShapeDtypeStruct((fields, rows, levels), BF16),
            jax.ShapeDtypeStruct((rows // 4, fields * levels), BF16),
            edge,
            edge,
        ],
        name="tendencies",
        compiler_params=pltpu.CompilerParams(vmem_limit_bytes=56 << 20),
    )(x, mass, jnp.asarray(quad), deriv, pick)


def section_body(
    t_ref, x_ref, m_ref, q_ref, left_ref, right_ref, o_ref, head_ref, tail_ref, inv_ref, rim_ref, *, per
):
    rows = x_ref.shape[1]
    span = per * 16
    count = rows // span
    fields = head_ref.shape[0] - 1
    s = lax.broadcasted_iota(jnp.int32, (per, 8, 128), 1)
    low = s < 4
    first = s % 4 == 0
    last = s % 4 == 3
    f = pl.program_id(0)

    def halves(v):
        v = v.reshape(per, 2, 8, 128)
        return v[:, 0], v[:, 1]

    def window(a):
        return pl.ds(pl.multiple_of(a * span, span), span)

    def across(here, a, k):
        at = pl.ds(pl.multiple_of(a * 8, 8), 8)
        left = left_ref[k, at, :].astype(F32)[None]
        right = right_ref[k, at, :].astype(F32)[None]
        result = []
        for h, p in enumerate(here):
            near = jnp.where(first[:1], left if h == 0 else roll(left, 7), 0.0)
            far = jnp.where(last[:1], roll(right, 3 - h), 0.0)
            up = jnp.where(last, roll(p, 3), 0.0)
            down = jnp.where(first, roll(p, 5), 0.0)
            up = jnp.concatenate([up[1:], far], axis=0)
            down = jnp.concatenate([near, down[:-1]], axis=0)
            result.append(p + up + down)
        return result

    def rims(k, p0, p1):
        both = jnp.concatenate([p0.reshape(per * 8, 128), p1.reshape(per * 8, 128)], axis=0).astype(BF16)
        if isinstance(k, int):
            rim_ref[...] = both
        else:
            o_ref[0, rows : rows + per * 16, :] = both
            o_ref[0, rows + per * 16 :, :] = rim_ref[...]
        p0 = p0.reshape(per // 2, 2, 8, 128)
        p1 = p1.reshape(per // 2, 2, 8, 128)
        half = low[: per // 2]
        head_ref[k] = (
            jnp.where(half, p0[:, 0], roll(p0[:, 1], 4)).reshape(per * 4, 128).astype(BF16)
        )
        tail_ref[k] = (
            jnp.where(half, roll(p1[:, 0], 4), p1[:, 1]).reshape(per * 4, 128).astype(BF16)
        )

    def sweep(load, k, put):
        start, p1 = across(load(0), 0, k)

        def step(a, carry):
            y0, before = carry
            p0, p1 = across(load(a), a, k)
            put(a - 1, y0, before + jnp.where(low, 0.0, roll(p0, 4)))
            return p0 + jnp.where(low, roll(before, 4), 0.0), p1

        y0, p1 = lax.fori_loop(1, count, step, (start, p1))
        put(count - 1, y0, p1)
        rims(k, start, p1)

    def joined(y0, y1):
        return jnp.stack([y0, y1], axis=1).reshape(span, 128)

    @pl.when(f == 0)
    def _():
        def mass_at(a):
            m0, m1 = halves(m_ref[window(a), :])
            return m0 * q_ref[0][None], m1 * q_ref[1][None]

        def put(a, y0, y1):
            inv_ref[window(a), :] = section_step / joined(y0, y1)

        sweep(mass_at, fields, put)
        top = pl.ds(0, span)
        v0, v1 = halves(inv_ref[top, :])
        inv_ref[top, :] = joined(jnp.zeros_like(v0), v1)
        end = pl.ds(rows - span, span)
        v0, v1 = halves(inv_ref[end, :])
        inv_ref[end, :] = joined(v0, jnp.zeros_like(v1))

    def put(a, y0, y1):
        y = x_ref[0, window(a), :] + joined(y0, y1) * inv_ref[window(a), :]
        o_ref[0, window(a), :] = y.astype(o_ref.dtype)

    sweep(lambda a: halves(t_ref[0, window(a), :].astype(F32)), f, put)


def section_of(t, x, mass, left, right, rows_a):
    fields, rows, levels = x.shape
    per = rows // rows_a // 16
    whole = lambda a: pl.BlockSpec(a.shape, lambda f: (0,) * a.ndim)
    quad = jnp.asarray(row_tables()[12:14])
    one = pl.BlockSpec((1, rows, levels), lambda f: (f, 0, 0))
    edge = jax.ShapeDtypeStruct((fields + 1, per * 4, levels), BF16)
    tall = rows + per * 32
    return pl.pallas_call(
        lambda *refs: section_body(*refs, per=per),
        grid=(fields,),
        in_specs=[one, one] + [whole(a) for a in (mass, quad, left, right)],
        out_specs=[
            pl.BlockSpec((1, tall, levels), lambda f: (f, 0, 0)),
            whole(edge),
            whole(edge),
        ],
        out_shape=[
            jax.ShapeDtypeStruct((fields, tall, levels), BF16),
            edge,
            edge,
        ],
        scratch_shapes=[pltpu.VMEM((rows, levels), F32), pltpu.VMEM((per * 16, levels), BF16)],
        name="section",
        compiler_params=pltpu.CompilerParams(vmem_limit_bytes=56 << 20),
    )(t, x, mass, quad, left, right)


def places_body(owner_ref, o_ref, *, devices, capacity):
    cols = owner_ref.shape[0]
    owner = owner_ref[...]
    hits = owner == lax.broadcasted_iota(jnp.int32, (cols, devices), 1)
    hits = jnp.where(hits, 1.0, 0.0)
    before = lax.broadcasted_iota(jnp.int32, (cols, cols), 0) > lax.broadcasted_iota(
        jnp.int32, (cols, cols), 1
    )
    before = jnp.where(before, 1.0, 0.0).astype(BF16)
    earlier = jnp.dot(before, hits.astype(BF16), preferred_element_type=F32)
    slot = jnp.sum(hits * earlier, axis=1, keepdims=True).astype(jnp.int32)
    o_ref[...] = owner * capacity + slot


def places(owner, devices, capacity):
    return pl.pallas_call(
        lambda a, o: places_body(a, o, devices=devices, capacity=capacity),
        out_shape=jax.ShapeDtypeStruct(owner.shape, jnp.int32),
        name="places",
        compiler_params=pltpu.CompilerParams(vmem_limit_bytes=60 << 20),
    )(owner)


def first_body(s_ref, w_ref, b_ref, wo_ref, o_ref, w2_ref, *, padded):
    width = s_ref.shape[1]
    rest = w_ref.shape[0] - width
    y = jnp.dot(s_ref[...], w_ref[:width, :], preferred_element_type=F32) + b_ref[...]
    o_ref[...] = y.astype(BF16)
    w2_ref[:rest, :] = w_ref[width:, :]
    w2_ref[rest:padded, :] = jnp.zeros((padded - rest, w2_ref.shape[1]), BF16)
    w2_ref[padded:, :] = wo_ref[...]


def first_part(state, weight, bias, weight_out, padded):
    cols, width = state.shape
    depth, hidden = weight.shape
    block = weight_out.shape[1]
    tall = padded + block
    return pl.pallas_call(
        lambda *refs: first_body(*refs, padded=padded),
        grid=(hidden // block,),
        in_specs=[
            pl.BlockSpec((cols, width), lambda i: (0, 0)),
            pl.BlockSpec((depth, block), lambda i: (0, i)),
            pl.BlockSpec((1, block), lambda i: (0, i)),
            pl.BlockSpec((block, block), lambda i: (i, 0)),
        ],
        out_specs=[
            pl.BlockSpec((cols, block), lambda i: (0, i)),
            pl.BlockSpec((tall, block), lambda i: (0, i)),
        ],
        out_shape=[
            jax.ShapeDtypeStruct((cols, hidden), BF16),
            jax.ShapeDtypeStruct((tall, hidden), BF16),
        ],
        name="first_part",
        compiler_params=pltpu.CompilerParams(vmem_limit_bytes=56 << 20),
    )(state, weight, bias, weight_out)


def finish_body(
    home_ref, place_ref, w_hbm, part_hbm, bo_ref, x_hbm, above_ref, below_ref, out_hbm,
    w_ref, part_ref, x_ref, sel_ref, aux_ref, spread_ref, o_ref, sem, out_sem, *, block
):
    fields, rows, levels = o_ref.shape
    cols = place_ref.shape[0]
    per = above_ref.shape[1] // 4
    edge_rows = pl.ds(rows, per * 32)
    steps = cols // block
    half = home_ref.shape[1] // 2
    hidden_half = w_ref.shape[1] // 2

    def rows_of(k, scale=1):
        return pl.ds(k * block * scale, block * scale)

    def columns(k, width):
        return pl.ds(k * width, width)

    def jobs():
        for k in (0, 1):
            yield f"w{k}", w_hbm.at[:, columns(k, hidden_half)], w_ref.at[:, columns(k, hidden_half)]
        yield "edge", x_hbm.at[:, edge_rows, :], x_ref.at[:, edge_rows, :]
        for k in range(steps):
            yield f"part{k}", part_hbm.at[rows_of(k), :], part_ref.at[rows_of(k), :]
            yield f"x{k}", x_hbm.at[:, rows_of(k, 4), :], x_ref.at[:, rows_of(k, 4), :]

    def each(names, act):
        for n, (name, src, dst) in enumerate(jobs()):
            if name in names:
                act(pltpu.make_async_copy(src, dst, sem.at[n]))

    def fetch(*names):
        each(names, lambda copy: copy.start())

    def wait(*names):
        each(names, lambda copy: copy.wait())

    later = [f"{kind}{k}" for k in range(1, steps) for kind in ("part", "x")]
    fetch("w0", "w1", "part0", "edge", "x0", *later)

    low = lax.broadcasted_iota(jnp.int32, (per // 2, 8, 128), 1) < 4

    def patch(h, halo, start):
        def total(k):
            p = halo[k].astype(F32).reshape(per // 2, 8, 128)
            q = roll(p, 4)
            if h == 0:
                add = jnp.stack([jnp.where(low, p, 0.0), jnp.where(low, q, 0.0)], axis=1)
            else:
                add = jnp.stack([jnp.where(low, 0.0, q), jnp.where(low, 0.0, p)], axis=1)
            own = pl.ds(rows + (per * 16 if k == fields else 0) + h * per * 8, per * 8)
            own = x_ref[0 if k == fields else k, own, :].astype(F32)
            return own.reshape(per, 8, 128) + add.reshape(per, 8, 128)

        scale = section_step / total(fields)
        to = pl.ds(start, per * 16)
        for f in range(fields):
            gain = total(f) * scale
            none = jnp.zeros_like(gain)
            both = jnp.stack([gain, none] if h == 0 else [none, gain], axis=1)
            o_ref[f, to, :] = o_ref[f, to, :] + both.reshape(per * 16, 128)

    wide = lax.broadcasted_iota(jnp.int32, (block, sel_ref.shape[1]), 1)
    for k in range(steps):
        sel_ref[rows_of(k), :] = jnp.where(place_ref[rows_of(k), :] == wide, 1.0, 0.0).astype(BF16)
    def gather(k, carry):
        lanes = pl.ds(pl.multiple_of(k * half, 128), half)
        aux_ref[:, lanes] = jnp.dot(
            sel_ref[...], home_ref[:, lanes], preferred_element_type=F32
        ).astype(BF16)
        return carry

    lax.fori_loop(0, 2, gather, 0)
    group = 128
    row = lax.broadcasted_iota(jnp.int32, (group * 4, group), 0)
    cell = (row // 16) * 4 + ((row // 8) % 2) * 2 + (row % 4) // 2
    spread = jnp.where(cell == lax.broadcasted_iota(jnp.int32, cell.shape, 1), 1.0, 0.0).astype(BF16)
    spread_ref[...] = spread
    padded = home_ref.shape[1]
    width = bo_ref.shape[1]
    wait("w0", "w1", "part0", "edge")

    def out_copy(k):
        at = pl.ds(pl.multiple_of(k * group * 4, group * 4), group * 4)
        return pltpu.make_async_copy(o_ref.at[:, at, :], out_hbm.at[:, at, :], out_sem.at[k])

    def layers(k, carry):
        at = pl.ds(pl.multiple_of(k * block, block), block)

        @pl.when(k == 1)
        def _():
            wait(*[f"part{m}" for m in range(1, steps)])

        v = part_ref[at, :].astype(F32) + jnp.dot(
            aux_ref[at, :], w_ref[:padded, :], preferred_element_type=F32
        )
        v = 0.5 * v
        hidden = (v + v * jnp.tanh(v)).astype(BF16)
        inc = bo_ref[...]
        for n in range(hidden.shape[1] // width):
            lanes = slice(n * width, (n + 1) * width)
            inc = inc + jnp.dot(hidden[:, lanes], w_ref[padded:, lanes], preferred_element_type=F32)
        inc = inc.astype(BF16)

        @pl.when(k == 0)
        def _():
            wait(*[f"x{m}" for m in range(steps)])

        for g in range(block // group):
            wide = jnp.dot(
                spread_ref[...], inc[g * group : (g + 1) * group], preferred_element_type=F32
            )
            to = pl.ds(pl.multiple_of((k * block + g * group) * 4, group * 4), group * 4)
            for f in range(fields):
                o_ref[f, to, :] = x_ref[f, to, :].astype(F32) + wide[:, f * levels : (f + 1) * levels]
            if g == 0:

                @pl.when(k == 0)
                def _():
                    patch(0, above_ref, 0)

            if g == block // group - 1:

                @pl.when(k == steps - 1)
                def _():
                    patch(1, below_ref, rows - per * 16)

            out_copy(k * (block // group) + g).start()

        return carry

    lax.fori_loop(0, steps, layers, 0)
    for g in range(cols // group):
        out_copy(g).wait()


def finish(home, place, weights, part, bias_out, x, above, below):
    cols, slots = place.shape[0], home.shape[0]
    fields, levels = x.shape[0], x.shape[2]
    result = (fields, cols * 4, levels)
    block = 384
    steps = cols // block
    far = pl.BlockSpec(memory_space=pl.ANY)
    near = pl.BlockSpec(memory_space=pltpu.VMEM)
    return pl.pallas_call(
        lambda *refs: finish_body(*refs, block=block),
        in_specs=[near, near, far, far, near, far, near, near],
        out_specs=far,
        out_shape=jax.ShapeDtypeStruct(result, F32),
        scratch_shapes=[pltpu.VMEM(a.shape, a.dtype) for a in (weights, part, x)]
        + [
            pltpu.VMEM((cols, slots), BF16),
            pltpu.VMEM((cols, home.shape[1]), BF16),
            pltpu.VMEM((512, 128), BF16),
            pltpu.VMEM(result, F32),
            pltpu.SemaphoreType.DMA((3 + 2 * steps,)),
            pltpu.SemaphoreType.DMA((cols // 128,)),
        ],
        name="finish",
        compiler_params=pltpu.CompilerParams(vmem_limit_bytes=48 << 20),
    )(home, place, weights, part, bias_out, x, above, below)


def shards(
    prognostic, layer_mass, column_aux, group_owner, weight_in, bias_in, weight_out, bias_out
):
    fields, rows_a, rows_b, _, _, levels = prognostic.shape
    n_curve, n_sub = lax.axis_size("curve"), lax.axis_size("sub")
    devices = n_curve * n_sub
    capacity = column_aux.shape[0] // devices
    aux_width = column_aux.shape[1]
    padded = -(-aux_width // 128) * 128
    rows = rows_a * rows_b * 16

    home = turn(column_aux.T, padded).reshape(devices, capacity, padded)
    home = lax.all_to_all(home, AXES, split_axis=0, concat_axis=0, tiled=True)
    home = home.reshape(devices * capacity, padded)

    x = prognostic.reshape(fields, rows, levels)
    mass = layer_mass.reshape(rows, levels)
    tend, state, left_out, right_out = tendencies(x, mass, rows_a)

    def ahead(n):
        return [(i, (i + 1) % n) for i in range(n)]

    def back(n):
        return [((i + 1) % n, i) for i in range(n)]

    left = lax.ppermute(right_out, "sub", ahead(n_sub))
    right = lax.ppermute(left_out, "sub", back(n_sub))
    section, head, tail = section_of(tend, x, mass, left, right, rows_a)
    above = lax.ppermute(tail, "curve", ahead(n_curve))
    below = lax.ppermute(head, "curve", back(n_curve))

    place = places(group_owner, devices, capacity)
    part, weights = first_part(state, weight_in, bias_in[None], weight_out, padded)
    out = finish(home, place, weights, part, bias_out[None], section, above, below)
    return out.reshape(prognostic.shape)


def solution(mesh):
    return jax.shard_map(
        shards,
        mesh=mesh,
        in_specs=(
            P(None, "curve", "sub", None, None, None),
            P("curve", "sub", None, None, None),
            P(("curve", "sub"), None),
            P(("curve", "sub"), None),
            P(),
            P(),
            P(),
            P(),
        ),
        out_specs=P(None, "curve", "sub", None, None, None),
        check_vma=False,
    )
```

```python
import jax
import jax.numpy as jnp
import numpy as np
from jax import lax
from jax.experimental import pallas as pl
from jax.experimental.pallas import tpu as pltpu
from jax.sharding import PartitionSpec as P

section_step = 0.1
AXES = ("curve", "sub")
F32 = jnp.float32
BF16 = jnp.bfloat16


def node_tables():
    nodes = np.array([-1.0, -1.0 / np.sqrt(5.0), 1.0 / np.sqrt(5.0), 1.0])
    quadrature = np.array([1.0 / 6.0, 5.0 / 6.0, 5.0 / 6.0, 1.0 / 6.0])
    products = np.array(
        [np.prod([nodes[i] - nodes[k] for k in range(4) if k != i]) for i in range(4)]
    )
    derivative = np.zeros((4, 4))
    for i in range(4):
        for k in range(4):
            if i != k:
                derivative[i, k] = products[i] / (products[k] * (nodes[i] - nodes[k]))
            else:
                derivative[i, i] = sum(1.0 / (nodes[i] - nodes[m]) for m in range(4) if m != i)
    return derivative.astype(np.float32), quadrature.astype(np.float32)


def row_tables():
    d, w = node_tables()
    s = np.arange(8)
    i, j = s // 4, s % 4
    tables = []
    for half in (0, 2):
        for column in (i, 1 - i, 2 + i, 3 - i):
            tables.append(-d[half + i, column])
    for shift in range(4):
        tables.append(-d[j, (j - shift) % 4])
    for half in (0, 2):
        tables.append(w[half + i] * w[j])
    return np.repeat(np.stack(tables)[:, :, None], 128, axis=2).astype(np.float32)


def lane_rows(x):
    return lax.broadcasted_iota(jnp.int32, x, len(x) - 2)


def roll(x, shift):
    return pltpu.roll(x, shift % 8, axis=1)


def turn_body(x_hbm, o_hbm, x_ref, o_ref, in_sem, out_sem):
    pieces = in_sem.shape[0]
    width, rows = x_ref.shape
    n = rows // pieces

    def take(k):
        lanes = pl.ds(k * n, n)
        return pltpu.make_async_copy(x_hbm.at[:, lanes], x_ref.at[:, lanes], in_sem.at[k])

    def give(k):
        at = pl.ds(k * n, n)
        return pltpu.make_async_copy(o_ref.at[at, :], o_hbm.at[at, :], out_sem.at[k])

    for k in range(pieces):
        take(k).start()
    o_ref[:, width:] = jnp.zeros((rows, o_ref.shape[1] - width), BF16)
    for k in range(pieces):
        take(k).wait()
        at = slice(k * n, (k + 1) * n)
        o_ref[at, :width] = x_ref[:, at].T
        give(k).start()
    for k in range(pieces):
        give(k).wait()


def turn(aux_t, padded):
    width, rows = aux_t.shape
    pieces = 6
    far = pl.BlockSpec(memory_space=pltpu.HBM)
    return pl.pallas_call(
        turn_body,
        in_specs=[far],
        out_specs=far,
        out_shape=jax.ShapeDtypeStruct((rows, padded), BF16),
        scratch_shapes=[
            pltpu.VMEM((width, rows), BF16),
            pltpu.VMEM((rows, padded), BF16),
            pltpu.SemaphoreType.DMA((pieces,)),
            pltpu.SemaphoreType.DMA((pieces,)),
        ],
        name="turn",
        compiler_params=pltpu.CompilerParams(vmem_limit_bytes=56 << 20),
    )(aux_t)


def tend_body(x_ref, m_ref, q_ref, deriv_ref, pick_ref, o_ref, c_ref, l_ref, r_ref):
    fields, rows, levels = x_ref.shape
    group = q_ref.shape[0]
    cells = group // 4
    lines = (pick_ref.shape[0] - cells) // 2

    for g in range(rows // group):
        at = pl.ds(g * group, group)
        cell_at = pl.ds(g * cells, cells)
        line_at = pl.ds(g * lines, lines)

        def picked(first, second):
            y = jnp.dot(
                pick_ref[...], jnp.concatenate([first, second], axis=1), preferred_element_type=F32
            )
            return y[:cells, :levels], y[cells:, levels:].astype(BF16)

        w = m_ref[at, :] * q_ref[...]
        wb = w.astype(BF16)
        mass, edge = picked(wb, wb)
        inv = 1.0 / mass
        l_ref[fields, line_at, :] = edge[:lines]
        r_ref[fields, line_at, :] = edge[lines:]
        uw = x_ref[0, at, :] * w
        vw = x_ref[1, at, :] * w
        for pair in range(0, fields, 2):
            both = (x_ref[pair, at, :], x_ref[pair + 1, at, :])
            high = jnp.concatenate([x.astype(BF16) for x in both], axis=1)
            low = jnp.concatenate([(x - x.astype(BF16).astype(F32)).astype(BF16) for x in both], axis=1)
            d = jnp.dot(
                deriv_ref[...], jnp.concatenate([high, high, low], axis=0), preferred_element_type=F32
            )
            for k, x in enumerate(both):
                f = pair + k
                lanes = slice(k * levels, (k + 1) * levels)
                out = (uw * d[:group, lanes] + vw * d[group:, lanes]).astype(BF16)
                xw = (uw if f == 0 else vw if f == 1 else x * w).astype(BF16)
                o_ref[f, at, :] = out
                mean, edge = picked(xw, out)
                c_ref[cell_at, f * levels : (f + 1) * levels] = (mean * inv).astype(BF16)
                l_ref[f, line_at, :] = edge[:lines]
                r_ref[f, line_at, :] = edge[lines:]


def derivative_table(group):
    d = node_tables()[0]
    r = np.arange(group)
    same = (r[:, None] // 16) == (r[None, :] // 16)
    i, j = (r // 4) % 4, r % 4
    along_first = np.where(same & (j[:, None] == j[None, :]), d[i[:, None], i[None, :]], 0.0)
    along_second = np.where(same & (i[:, None] == i[None, :]), d[j[:, None], j[None, :]], 0.0)
    return -np.concatenate([along_first, along_second], axis=0)


def pick_table(group, span):
    r = np.arange(group)
    cells = np.zeros((group // 4, group), np.float32)
    cells[(r // 16) * 4 + ((r // 8) % 2) * 2 + (r % 4) // 2, r] = 1.0
    lines = [np.zeros((group // span * 8, group), np.float32) for _ in range(2)]
    for a in range(group // span):
        for i in range(4):
            to = a * 8 + (i % 2) * 4 + i // 2
            lines[0][to, a * span + i * 4] = 1.0
            lines[1][to, (a + 1) * span - 16 + i * 4 + 3] = 1.0
    return np.concatenate([cells] + lines, axis=0)


def tendencies(x, mass, rows_a):
    fields, rows, levels = x.shape
    span = rows // rows_a
    group = 2 * span
    lot = 4
    block = lot * span
    quad = np.tile(row_tables()[12:14].reshape(16, 128), (group // 16, 1))
    deriv = derivative_table(group)
    top = deriv.astype(jnp.bfloat16)
    deriv = jnp.asarray(np.concatenate([top, (deriv - top.astype(np.float64)).astype(jnp.bfloat16), top], axis=1))
    pick = jnp.asarray(pick_table(group, span), BF16)
    edge = jax.ShapeDtypeStruct((fields + 1, rows_a * 8, levels), BF16)
    whole = lambda a: pl.BlockSpec(a.shape, lambda i: (0, 0))
    return pl.pallas_call(
        tend_body,
        grid=(rows // block,),
        in_specs=[
            pl.BlockSpec((fields, block, levels), lambda i: (0, i, 0)),
            pl.BlockSpec((block, levels), lambda i: (i, 0)),
            whole(quad),
            whole(deriv),
            whole(pick),
        ],
        out_specs=[
            pl.BlockSpec((fields, block, levels), lambda i: (0, i, 0)),
            pl.BlockSpec((block // 4, fields * levels), lambda i: (i, 0)),
            pl.BlockSpec((fields + 1, lot * 8, levels), lambda i: (0, i, 0)),
            pl.BlockSpec((fields + 1, lot * 8, levels), lambda i: (0, i, 0)),
        ],
        out_shape=[
            jax.ShapeDtypeStruct((fields, rows, levels), BF16),
            jax.ShapeDtypeStruct((rows // 4, fields * levels), BF16),
            edge,
            edge,
        ],
        name="tendencies",
        compiler_params=pltpu.CompilerParams(vmem_limit_bytes=56 << 20),
    )(x, mass, jnp.asarray(quad), deriv, pick)


def section_body(
    t_ref, x_ref, m_ref, q_ref, left_ref, right_ref, o_ref, head_ref, tail_ref, inv_ref, rim_ref, *, per
):
    rows = x_ref.shape[1]
    span = per * 16
    count = rows // span
    fields = head_ref.shape[0] - 1
    s = lax.broadcasted_iota(jnp.int32, (per, 8, 128), 1)
    low = s < 4
    first = s % 4 == 0
    last = s % 4 == 3
    f = pl.program_id(0)

    def halves(v):
        v = v.reshape(per, 2, 8, 128)
        return v[:, 0], v[:, 1]

    def window(a):
        return pl.ds(pl.multiple_of(a * span, span), span)

    def across(here, a, k):
        at = pl.ds(pl.multiple_of(a * 8, 8), 8)
        left = left_ref[k, at, :].astype(F32)[None]
        right = right_ref[k, at, :].astype(F32)[None]
        result = []
        for h, p in enumerate(here):
            near = jnp.where(first[:1], left if h == 0 else roll(left, 7), 0.0)
            far = jnp.where(last[:1], roll(right, 3 - h), 0.0)
            up = jnp.where(last, roll(p, 3), 0.0)
            down = jnp.where(first, roll(p, 5), 0.0)
            up = jnp.concatenate([up[1:], far], axis=0)
            down = jnp.concatenate([near, down[:-1]], axis=0)
            result.append(p + up + down)
        return result

    def rims(k, p0, p1):
        both = jnp.concatenate([p0.reshape(per * 8, 128), p1.reshape(per * 8, 128)], axis=0).astype(BF16)
        if isinstance(k, int):
            rim_ref[...] = both
        else:
            o_ref[0, rows : rows + per * 16, :] = both
            o_ref[0, rows + per * 16 :, :] = rim_ref[...]
        p0 = p0.reshape(per // 2, 2, 8, 128)
        p1 = p1.reshape(per // 2, 2, 8, 128)
        half = low[: per // 2]
        head_ref[k] = (
            jnp.where(half, p0[:, 0], roll(p0[:, 1], 4)).reshape(per * 4, 128).astype(BF16)
        )
        tail_ref[k] = (
            jnp.where(half, roll(p1[:, 0], 4), p1[:, 1]).reshape(per * 4, 128).astype(BF16)
        )

    def sweep(load, k, put):
        start, p1 = across(load(0), 0, k)

        def step(a, carry):
            y0, before = carry
            p0, p1 = across(load(a), a, k)
            put(a - 1, y0, before + jnp.where(low, 0.0, roll(p0, 4)))
            return p0 + jnp.where(low, roll(before, 4), 0.0), p1

        y0, p1 = lax.fori_loop(1, count, step, (start, p1))
        put(count - 1, y0, p1)
        rims(k, start, p1)

    def joined(y0, y1):
        return jnp.stack([y0, y1], axis=1).reshape(span, 128)

    @pl.when(f == 0)
    def _():
        def mass_at(a):
            m0, m1 = halves(m_ref[window(a), :])
            return m0 * q_ref[0][None], m1 * q_ref[1][None]

        def put(a, y0, y1):
            inv_ref[window(a), :] = section_step / joined(y0, y1)

        sweep(mass_at, fields, put)
        top = pl.ds(0, span)
        v0, v1 = halves(inv_ref[top, :])
        inv_ref[top, :] = joined(jnp.zeros_like(v0), v1)
        end = pl.ds(rows - span, span)
        v0, v1 = halves(inv_ref[end, :])
        inv_ref[end, :] = joined(v0, jnp.zeros_like(v1))

    def put(a, y0, y1):
        y = x_ref[0, window(a), :] + joined(y0, y1) * inv_ref[window(a), :]
        o_ref[0, window(a), :] = y.astype(o_ref.dtype)

    sweep(lambda a: halves(t_ref[0, window(a), :].astype(F32)), f, put)


def section_of(t, x, mass, left, right, rows_a):
    fields, rows, levels = x.shape
    per = rows // rows_a // 16
    whole = lambda a: pl.BlockSpec(a.shape, lambda f: (0,) * a.ndim)
    quad = jnp.asarray(row_tables()[12:14])
    one = pl.BlockSpec((1, rows, levels), lambda f: (f, 0, 0))
    edge = jax.ShapeDtypeStruct((fields + 1, per * 4, levels), BF16)
    tall = rows + per * 32
    return pl.pallas_call(
        lambda *refs: section_body(*refs, per=per),
        grid=(fields,),
        in_specs=[one, one] + [whole(a) for a in (mass, quad, left, right)],
        out_specs=[
            pl.BlockSpec((1, tall, levels), lambda f: (f, 0, 0)),
            whole(edge),
            whole(edge),
        ],
        out_shape=[
            jax.ShapeDtypeStruct((fields, tall, levels), BF16),
            edge,
            edge,
        ],
        scratch_shapes=[pltpu.VMEM((rows, levels), F32), pltpu.VMEM((per * 16, levels), BF16)],
        name="section",
        compiler_params=pltpu.CompilerParams(vmem_limit_bytes=56 << 20),
    )(t, x, mass, quad, left, right)


def places_body(owner_ref, o_ref, *, devices, capacity):
    cols = owner_ref.shape[0]
    owner = owner_ref[...]
    hits = owner == lax.broadcasted_iota(jnp.int32, (cols, devices), 1)
    hits = jnp.where(hits, 1.0, 0.0)
    before = lax.broadcasted_iota(jnp.int32, (cols, cols), 0) > lax.broadcasted_iota(
        jnp.int32, (cols, cols), 1
    )
    before = jnp.where(before, 1.0, 0.0).astype(BF16)
    earlier = jnp.dot(before, hits.astype(BF16), preferred_element_type=F32)
    slot = jnp.sum(hits * earlier, axis=1, keepdims=True).astype(jnp.int32)
    o_ref[...] = owner * capacity + slot


def places(owner, devices, capacity):
    return pl.pallas_call(
        lambda a, o: places_body(a, o, devices=devices, capacity=capacity),
        out_shape=jax.ShapeDtypeStruct(owner.shape, jnp.int32),
        name="places",
        compiler_params=pltpu.CompilerParams(vmem_limit_bytes=60 << 20),
    )(owner)


def first_body(s_ref, w_ref, b_ref, wo_ref, o_ref, w2_ref, *, padded):
    width = s_ref.shape[1]
    rest = w_ref.shape[0] - width
    y = jnp.dot(s_ref[...], w_ref[:width, :], preferred_element_type=F32) + b_ref[...]
    o_ref[...] = y.astype(BF16)
    w2_ref[:rest, :] = w_ref[width:, :]
    w2_ref[rest:padded, :] = jnp.zeros((padded - rest, w2_ref.shape[1]), BF16)
    w2_ref[padded:, :] = wo_ref[...]


def first_part(state, weight, bias, weight_out, padded):
    cols, width = state.shape
    depth, hidden = weight.shape
    block = weight_out.shape[1]
    tall = padded + block
    return pl.pallas_call(
        lambda *refs: first_body(*refs, padded=padded),
        grid=(hidden // block,),
        in_specs=[
            pl.BlockSpec((cols, width), lambda i: (0, 0)),
            pl.BlockSpec((depth, block), lambda i: (0, i)),
            pl.BlockSpec((1, block), lambda i: (0, i)),
            pl.BlockSpec((block, block), lambda i: (i, 0)),
        ],
        out_specs=[
            pl.BlockSpec((cols, block), lambda i: (0, i)),
            pl.BlockSpec((tall, block), lambda i: (0, i)),
        ],
        out_shape=[
            jax.ShapeDtypeStruct((cols, hidden), BF16),
            jax.ShapeDtypeStruct((tall, hidden), BF16),
        ],
        name="first_part",
        compiler_params=pltpu.CompilerParams(vmem_limit_bytes=56 << 20),
    )(state, weight, bias, weight_out)


def finish_body(
    home_ref, place_ref, w_hbm, part_hbm, bo_ref, x_hbm, above_ref, below_ref, out_hbm,
    w_ref, part_ref, x_ref, sel_ref, aux_ref, spread_ref, o_ref, sem, out_sem, *, block
):
    fields, rows, levels = o_ref.shape
    cols = place_ref.shape[0]
    per = above_ref.shape[1] // 4
    edge_rows = pl.ds(rows, per * 32)
    steps = cols // block
    half = home_ref.shape[1] // 2
    hidden_half = w_ref.shape[1] // 2

    def rows_of(k, scale=1):
        return pl.ds(k * block * scale, block * scale)

    def columns(k, width):
        return pl.ds(k * width, width)

    def jobs():
        for k in (0, 1):
            yield f"w{k}", w_hbm.at[:, columns(k, hidden_half)], w_ref.at[:, columns(k, hidden_half)]
        yield "edge", x_hbm.at[:, edge_rows, :], x_ref.at[:, edge_rows, :]
        for k in range(steps):
            yield f"part{k}", part_hbm.at[rows_of(k), :], part_ref.at[rows_of(k), :]
            yield f"x{k}", x_hbm.at[:, rows_of(k, 4), :], x_ref.at[:, rows_of(k, 4), :]

    def each(names, act):
        for n, (name, src, dst) in enumerate(jobs()):
            if name in names:
                act(pltpu.make_async_copy(src, dst, sem.at[n]))

    def fetch(*names):
        each(names, lambda copy: copy.start())

    def wait(*names):
        each(names, lambda copy: copy.wait())

    later = [f"{kind}{k}" for k in range(1, steps) for kind in ("part", "x")]
    fetch("w0", "w1", "part0", "edge", "x0", *later)

    low = lax.broadcasted_iota(jnp.int32, (per // 2, 8, 128), 1) < 4

    def patch(h, halo, start):
        def total(k):
            p = halo[k].astype(F32).reshape(per // 2, 8, 128)
            q = roll(p, 4)
            if h == 0:
                add = jnp.stack([jnp.where(low, p, 0.0), jnp.where(low, q, 0.0)], axis=1)
            else:
                add = jnp.stack([jnp.where(low, 0.0, q), jnp.where(low, 0.0, p)], axis=1)
            own = pl.ds(rows + (per * 16 if k == fields else 0) + h * per * 8, per * 8)
            own = x_ref[0 if k == fields else k, own, :].astype(F32)
            return own.reshape(per, 8, 128) + add.reshape(per, 8, 128)

        scale = section_step / total(fields)
        to = pl.ds(start, per * 16)
        for f in range(fields):
            gain = total(f) * scale
            none = jnp.zeros_like(gain)
            both = jnp.stack([gain, none] if h == 0 else [none, gain], axis=1)
            o_ref[f, to, :] = o_ref[f, to, :] + both.reshape(per * 16, 128)

    wide = lax.broadcasted_iota(jnp.int32, (block, sel_ref.shape[1]), 1)
    for k in range(steps):
        sel_ref[rows_of(k), :] = jnp.where(place_ref[rows_of(k), :] == wide, 1.0, 0.0).astype(BF16)
    def gather(k, carry):
        lanes = pl.ds(pl.multiple_of(k * half, 128), half)
        aux_ref[:, lanes] = jnp.dot(
            sel_ref[...], home_ref[:, lanes], preferred_element_type=F32
        ).astype(BF16)
        return carry

    lax.fori_loop(0, 2, gather, 0)
    group = 128
    row = lax.broadcasted_iota(jnp.int32, (group * 4, group), 0)
    cell = (row // 16) * 4 + ((row // 8) % 2) * 2 + (row % 4) // 2
    spread = jnp.where(cell == lax.broadcasted_iota(jnp.int32, cell.shape, 1), 1.0, 0.0).astype(BF16)
    spread_ref[...] = spread
    padded = home_ref.shape[1]
    width = bo_ref.shape[1]
    wait("w0", "w1", "part0", "edge")

    def out_copy(k):
        at = pl.ds(pl.multiple_of(k * group * 4, group * 4), group * 4)
        return pltpu.make_async_copy(o_ref.at[:, at, :], out_hbm.at[:, at, :], out_sem.at[k])

    def layers(k, carry):
        at = pl.ds(pl.multiple_of(k * block, block), block)

        @pl.when(k == 1)
        def _():
            wait(*[f"part{m}" for m in range(1, steps)])

        v = part_ref[at, :].astype(F32) + jnp.dot(
            aux_ref[at, :], w_ref[:padded, :], preferred_element_type=F32
        )
        v = 0.5 * v
        hidden = (v + v * jnp.tanh(v)).astype(BF16)
        inc = bo_ref[...]
        for n in range(hidden.shape[1] // width):
            lanes = slice(n * width, (n + 1) * width)
            inc = inc + jnp.dot(hidden[:, lanes], w_ref[padded:, lanes], preferred_element_type=F32)
        inc = inc.astype(BF16)

        @pl.when(k == 0)
        def _():
            wait(*[f"x{m}" for m in range(steps)])

        for g in range(block // group):
            wide = jnp.dot(
                spread_ref[...], inc[g * group : (g + 1) * group], preferred_element_type=F32
            )
            to = pl.ds(pl.multiple_of((k * block + g * group) * 4, group * 4), group * 4)
            for f in range(fields):
                o_ref[f, to, :] = x_ref[f, to, :].astype(F32) + wide[:, f * levels : (f + 1) * levels]
            if g == 0:

                @pl.when(k == 0)
                def _():
                    patch(0, above_ref, 0)

            if g == block // group - 1:

                @pl.when(k == steps - 1)
                def _():
                    patch(1, below_ref, rows - per * 16)

            out_copy(k * (block // group) + g).start()

        return carry

    lax.fori_loop(0, steps, layers, 0)
    for g in range(cols // group):
        out_copy(g).wait()


def finish(home, place, weights, part, bias_out, x, above, below):
    cols, slots = place.shape[0], home.shape[0]
    fields, levels = x.shape[0], x.shape[2]
    result = (fields, cols * 4, levels)
    block = 384
    steps = cols // block
    far = pl.BlockSpec(memory_space=pl.ANY)
    near = pl.BlockSpec(memory_space=pltpu.VMEM)
    return pl.pallas_call(
        lambda *refs: finish_body(*refs, block=block),
        in_specs=[near, near, far, far, near, far, near, near],
        out_specs=far,
        out_shape=jax.ShapeDtypeStruct(result, F32),
        scratch_shapes=[pltpu.VMEM(a.shape, a.dtype) for a in (weights, part, x)]
        + [
            pltpu.VMEM((cols, slots), BF16),
            pltpu.VMEM((cols, home.shape[1]), BF16),
            pltpu.VMEM((512, 128), BF16),
            pltpu.VMEM(result, F32),
            pltpu.SemaphoreType.DMA((3 + 2 * steps,)),
            pltpu.SemaphoreType.DMA((cols // 128,)),
        ],
        name="finish",
        compiler_params=pltpu.CompilerParams(vmem_limit_bytes=48 << 20),
    )(home, place, weights, part, bias_out, x, above, below)


def shards(
    prognostic, layer_mass, column_aux, group_owner, weight_in, bias_in, weight_out, bias_out
):
    fields, rows_a, rows_b, _, _, levels = prognostic.shape
    n_curve, n_sub = lax.axis_size("curve"), lax.axis_size("sub")
    devices = n_curve * n_sub
    capacity = column_aux.shape[0] // devices
    aux_width = column_aux.shape[1]
    padded = -(-aux_width // 128) * 128
    rows = rows_a * rows_b * 16

    home = turn(column_aux.T, padded).reshape(devices, capacity, padded)
    home = lax.all_to_all(home, AXES, split_axis=0, concat_axis=0, tiled=True)
    home = home.reshape(devices * capacity, padded)

    x = prognostic.reshape(fields, rows, levels)
    mass = layer_mass.reshape(rows, levels)
    tend, state, left_out, right_out = tendencies(x, mass, rows_a)

    def ahead(n):
        return [(i, (i + 1) % n) for i in range(n)]

    def back(n):
        return [((i + 1) % n, i) for i in range(n)]

    left = lax.ppermute(right_out, "sub", ahead(n_sub))
    right = lax.ppermute(left_out, "sub", back(n_sub))
    section, head, tail = section_of(tend, x, mass, left, right, rows_a)
    above = lax.ppermute(tail, "curve", ahead(n_curve))
    below = lax.ppermute(head, "curve", back(n_curve))

    place = places(group_owner, devices, capacity)
    part, weights = first_part(state, weight_in, bias_in[None], weight_out, padded)
    out = finish(home, place, weights, part, bias_out[None], section, above, below)
    return out.reshape(prognostic.shape)


def solution(mesh):
    return jax.shard_map(
        shards,
        mesh=mesh,
        in_specs=(
            P(None, "curve", "sub", None, None, None),
            P("curve", "sub", None, None, None),
            P(("curve", "sub"), None),
            P(("curve", "sub"), None),
            P(),
            P(),
            P(),
            P(),
        ),
        out_specs=P(None, "curve", "sub", None, None, None),
        check_vma=False,
    )
```
